128 devices in a mesh: member: 4 (over y, x), dp: 16 (over z), mp: 2 (over core).
Axes of the slice: x: 2, y: 2, z: 16, core: 2. Of those that a mesh axis runs over, the one named last changes fastest.
The devices are a block of a 8x8x16 slice.
Arguments:
- activations: bfloat16 [8192, 2048], P(('member', 'dp')), parts along dimension 0, may hold values from -6 to 6
- out_grads: bfloat16 [8192, 10240], P(('member', 'dp'), 'mp'), parts along dimension 0, may hold values from -0.19921875 to 0.19921875
- slot_table: int32 [8, 16], P(('member', 'mp')), parts along dimension 0, may hold values from 0 to 15, each once within a row
- exponent_index: int32 [8, 16], P(('member', 'mp')), parts along dimension 0, may hold values from 0 to 1
- damping_index: int32 [8, 16], P(('member', 'mp')), parts along dimension 0, may hold values from 0 to 3
Outputs:
- update: bfloat16 [8192, 10240], P('member', 'mp'), parts along dimension 0
- preconditioners: bfloat16 [8, 16, 2, 1024, 1024], P(('member', 'mp'), 'dp'), parts along dimension 0
The draws below stay inside these ranges and needn't reach their ends.
There are 4 independent parts, one for each index of `member`. The reference program is written for one: setup_inputs(seed, part) draws one part's arguments, and reference() takes and returns one part's arrays. A program takes and returns all parts, laid end to end along the dimension named above; each array names one. Nothing has to cross between parts.
Inputs may be any that keep to these rules, and one draw needn't show every extreme that they name: `slot_table`: each row is a permutation of 0 to 15; slot s belongs to dp index s.
All inputs are finite; a program needn't handle non-finite values.
Results may differ from the reference program's by a relative error of at most 0.006.
The reference program's roundings to bfloat16 on the way (of `gradient`, `half_step` and `assembled`) count: a program that leaves them out, or rounds other values in their place, can miss the bound.
Values may be sent and summed in bfloat16 or wider, within the bound.
A program may use at most 192 MiB of HBM per device.

```python
import jax
import jax.numpy as jnp
from jax import lax

D_WIN = 2048
FF_WIN = 10240
BLK = 1024
SLOTS = 16
ITERS = 2
TOKENS = 2048
N_MP = 2


def plant(entries, stream_key, least, top_value):
    index_at = [jax.random.randint(jax.random.fold_in(stream_key, axis), (), 0, length) for axis, length in enumerate(entries.shape)]
    widest = entries.shape.index(max(entries.shape))
    neighbour = index_at[:widest] + [(index_at[widest] + 1) % entries.shape[widest]] + index_at[widest + 1:]
    return entries.at[tuple(index_at)].set(least).at[tuple(neighbour)].set(top_value)


def block_levels(own_key, dims, cuts, low, top_value):
    factor_of, own = 1.0, jax.random.fold_in(own_key, 6)
    for dim, shards_of in cuts:
        heights = jnp.exp(jax.random.uniform(jax.random.fold_in(own, dim), (shards_of,), jnp.float32, low / len(cuts), top_value / len(cuts)))
        factor_of = factor_of * jnp.repeat(heights, dims[dim] // shards_of).reshape([-1 if axis == dim else 1 for axis in range(len(dims))])
    return factor_of


def gaussian(key, extent, width, bound, split=(), kind=jnp.bfloat16):
    array = width * jax.random.normal(key, extent, jnp.float32)
    if split:
        array = array * block_levels(key, extent, split, -0.22, 0.18)
    return jnp.clip(array, -bound, bound).astype(kind)


def setup_inputs(seed: int = 0, part: int = 0) -> dict:
    keys = jax.random.split(jax.random.key(seed), 6)
    part_keys = jax.random.split(jax.random.fold_in(keys[5], part), 6)
    activations = gaussian(part_keys[0], (TOKENS, D_WIN), 1.0, 6.0, ((0, 16),))
    out_grads = gaussian(part_keys[1], (TOKENS, FF_WIN), 0.03125, 0.19921875, ((0, 16), (1, 2)))
    slot_table = jax.vmap(lambda own: jax.random.permutation(own, SLOTS))(jax.random.split(part_keys[2], N_MP)).reshape((N_MP, SLOTS)).astype(jnp.int32)
    exponent_index = plant(jax.random.randint(part_keys[3], (N_MP, SLOTS), 0, 2), jax.random.fold_in(part_keys[3], 1), 0, 1).astype(jnp.int32)
    damping_index = plant(jax.random.randint(part_keys[4], (N_MP, SLOTS), 0, 4), jax.random.fold_in(part_keys[4], 1), 0, 3).astype(jnp.int32)
    return dict(activations=activations, out_grads=out_grads, slot_table=slot_table, exponent_index=exponent_index, damping_index=damping_index)


ROOT_ORDERS = (2.0, 4.0)
DAMPINGS = (0.03, 0.1, 0.3, 1.0)

def table_value(picked, values_table):
    values = jnp.asarray(values_table, jnp.float32)
    matches = jnp.arange(len(values_table), dtype=jnp.int32) == picked
    return jnp.sum(jnp.where(matches, values, 0.0))

def half_dot(first, second):
    return jnp.dot(first.astype(jnp.bfloat16), second.astype(jnp.bfloat16), preferred_element_type=jnp.float32)

def inverse_root(statistic, root_order, quartic, damping):
    dimension = statistic.shape[0]
    identity = jnp.eye(dimension, dtype=jnp.float32)
    damped = statistic + damping * (jnp.trace(statistic) / dimension + 1.0) * identity
    current = damped * (dimension / (2.0 * jnp.trace(damped)))
    factor = ((root_order + 1.0) * identity - current) / root_order
    estimate = factor
    for sweep in range(1, ITERS):
        square = half_dot(factor, factor)
        fourth = half_dot(square, square)
        raised = jnp.where(quartic, fourth, square)
        current = half_dot(raised, current)
        factor = ((root_order + 1.0) * identity - current) / root_order
        estimate = half_dot(estimate, factor)
    return estimate.astype(jnp.bfloat16)

def precondition(act_block, grad_block, root_order, quartic, damping):
    gradient = lax.dot_general(act_block, grad_block, (((0,), (0,)), ((), ())), preferred_element_type=jnp.float32).astype(jnp.bfloat16)
    left_stat = lax.dot_general(gradient, gradient, (((1,), (1,)), ((), ())), preferred_element_type=jnp.float32)
    right_stat = lax.dot_general(gradient, gradient, (((0,), (0,)), ((), ())), preferred_element_type=jnp.float32)
    left_root = inverse_root(left_stat, root_order, quartic, damping)
    right_root = inverse_root(right_stat, root_order, quartic, damping)
    half_step = jnp.dot(left_root, gradient, preferred_element_type=jnp.float32).astype(jnp.bfloat16)
    block_update = jnp.dot(half_step, right_root, preferred_element_type=jnp.float32).astype(jnp.bfloat16)
    return (block_update, jnp.stack([left_root, right_root]))

def reference(activations, out_grads, slot_table, exponent_index, damping_index):
    row_blocks = D_WIN // BLK
    col_blocks = FF_WIN // (N_MP * BLK)
    half_blocks = row_blocks * col_blocks
    acts_grid = activations.reshape(TOKENS, row_blocks, BLK)
    grads_grid = out_grads.reshape(TOKENS, N_MP, col_blocks, BLK)
    flat_exp = exponent_index.reshape(N_MP * SLOTS)
    flat_damp = damping_index.reshape(N_MP * SLOTS)

    def one_slot(flat_slot):
        half_id = flat_slot // SLOTS
        slot_id = flat_slot % SLOTS
        exp_pick = lax.dynamic_index_in_dim(flat_exp, flat_slot, 0, keepdims=False)
        damp_pick = lax.dynamic_index_in_dim(flat_damp, flat_slot, 0, keepdims=False)
        root_order = table_value(exp_pick, ROOT_ORDERS)
        quartic = exp_pick == 1
        damping = table_value(damp_pick, DAMPINGS)
        table_row = lax.dynamic_index_in_dim(slot_table, half_id, 0, keepdims=False)[:half_blocks]
        matches = table_row == slot_id
        filled = jnp.any(matches)
        block_id = jnp.sum(jnp.where(matches, jnp.arange(half_blocks, dtype=jnp.int32), 0)).astype(jnp.int32)
        act_block = lax.dynamic_index_in_dim(acts_grid, block_id // col_blocks, 1, keepdims=False)
        grad_half = lax.dynamic_index_in_dim(grads_grid, half_id, 1, keepdims=False)
        grad_block = lax.dynamic_index_in_dim(grad_half, block_id % col_blocks, 1, keepdims=False)
        act_block = jnp.where(filled, act_block, jnp.zeros_like(act_block))
        grad_block = jnp.where(filled, grad_block, jnp.zeros_like(grad_block))
        return precondition(act_block, grad_block, root_order, quartic, damping)
    block_updates, roots = lax.map(one_slot, jnp.arange(N_MP * SLOTS, dtype=jnp.int32))
    by_slot = block_updates.reshape(N_MP, SLOTS, BLK, BLK)
    chosen = jnp.take_along_axis(by_slot, slot_table[:, :half_blocks][:, :, None, None], axis=1)
    assembled = chosen.reshape(N_MP, row_blocks, col_blocks, BLK, BLK).transpose(1, 3, 0, 2, 4).reshape(D_WIN, FF_WIN)
    wide = assembled.astype(jnp.float32)
    total_sq = jnp.sum(wide * wide)
    rescale = lax.rsqrt(total_sq / (D_WIN * FF_WIN) + 1.0)
    update = (wide * rescale).astype(jnp.bfloat16)
    return (update, roots.reshape(N_MP, SLOTS, 2, BLK, BLK))
```

```python
import functools

import jax
import jax.numpy as jnp
import numpy as np
from jax import lax
from jax.experimental import pallas as pl
from jax.experimental.pallas import tpu as pltpu
from jax.sharding import PartitionSpec as P

BLK = 1024
LANE = 128
ROOT_ORDERS = (2.0, 4.0)
DAMPINGS = (0.03, 0.1, 0.3, 1.0)
SHIFT = 4
MESH = pl.DeviceIdType.MESH


def table_value(picked, values_table):
    values = jnp.asarray(values_table, jnp.float32)
    matches = jnp.arange(len(values_table), dtype=jnp.int32) == picked
    return jnp.sum(jnp.where(matches, values, 0.0))


def half_dot(first, second):
    return jnp.dot(
        first.astype(jnp.bfloat16), second.astype(jnp.bfloat16), preferred_element_type=jnp.float32
    )


def inverse_root(statistic, root_order, quartic, damping):
    dimension = statistic.shape[0]
    identity = jnp.eye(dimension, dtype=jnp.float32)
    damped = statistic + damping * (jnp.trace(statistic) / dimension + 1.0) * identity
    current = damped * (dimension / (2.0 * jnp.trace(damped)))
    factor = ((root_order + 1.0) * identity - current) / root_order
    estimate = factor
    square = half_dot(factor, factor)
    fourth = half_dot(square, square)
    raised = jnp.where(quartic, fourth, square)
    current = half_dot(raised, current)
    factor = ((root_order + 1.0) * identity - current) / root_order
    estimate = half_dot(estimate, factor)
    return estimate.astype(jnp.bfloat16)


def two_roots(gradient, exp_pick, damp_pick):
    root_order = table_value(exp_pick, ROOT_ORDERS)
    quartic = exp_pick == 1
    damping = table_value(damp_pick, DAMPINGS)
    left_stat = lax.dot_general(
        gradient, gradient, (((1,), (1,)), ((), ())), preferred_element_type=jnp.float32
    )
    right_stat = lax.dot_general(
        gradient, gradient, (((0,), (0,)), ((), ())), preferred_element_type=jnp.float32
    )
    return (
        inverse_root(left_stat, root_order, quartic, damping),
        inverse_root(right_stat, root_order, quartic, damping),
    )


def greet_group(n, z, h):
    barrier = pltpu.get_barrier_semaphore()
    pl.semaphore_signal(barrier, inc=1, device_id={"mp": 1 - h}, device_id_type=MESH)
    for o in range(1, n):
        for t in range(2):
            pl.semaphore_signal(
                barrier, inc=1, device_id={"dp": lax.rem(z + o, n), "mp": t}, device_id_type=MESH
            )
    pl.semaphore_wait(barrier, 2 * n - 1)


def remote(src, dst, send, recv, **to):
    return pltpu.make_async_remote_copy(
        src_ref=src, dst_ref=dst, send_sem=send, recv_sem=recv, device_id=to, device_id_type=MESH
    )


def collect_kernel(
    n, a_in, b_in, tbl_in, a_all, b_all, tbl_out,
    as_r, ar_r, as_l, ar_l, b_send, b_recv, f_send, f_recv, t_send, t_recv, loc_sem,
):
    z = lax.axis_index("dp")
    h = lax.axis_index("mp")
    tok = a_in.shape[0]
    half = tok // 2
    right, left = lax.rem(z + 1, n), lax.rem(z + n - 1, n)
    greet_group(n, z, h)
    steps = n // 2
    top, low = pl.ds(0, half), pl.ds(half, half)
    right_sends = []
    left_sends = []

    def ring_send(step):
        if step == 0:
            src_r = src_l = a_in
            at_r = at_l = z
        else:
            at_r = lax.rem(z + n - step, n)
            at_l = lax.rem(z + step, n)
            src_r, src_l = a_all.at[at_r], a_all.at[at_l]
        dst_r, dst_l = a_all.at[at_r], a_all.at[at_l]
        if step == steps - 1:
            src_r, dst_r = src_r.at[top], dst_r.at[top]
            src_l, dst_l = src_l.at[low], dst_l.at[low]
        one = remote(src_r, dst_r, as_r.at[step], ar_r.at[step], dp=right)
        two = remote(src_l, dst_l, as_l.at[step], ar_l.at[step], dp=left)
        one.start()
        two.start()
        right_sends.append(one)
        left_sends.append(two)

    def ring_recv(step):
        at_r = lax.rem(z + n - step - 1, n)
        at_l = lax.rem(z + step + 1, n)
        dst_r, dst_l = a_all.at[at_r], a_all.at[at_l]
        if step == steps - 1:
            dst_r, dst_l = dst_r.at[top], dst_l.at[low]
        remote(dst_r, dst_r, as_r.at[step], ar_r.at[step], dp=right).wait_recv()
        remote(dst_l, dst_l, as_l.at[step], ar_l.at[step], dp=left).wait_recv()

    table = remote(tbl_in, tbl_out, t_send, t_recv, mp=1 - h)
    table.start()
    own = pltpu.make_async_copy(a_in, a_all.at[z], loc_sem)
    own.start()
    ring_send(0)
    parity = lax.rem(z + h, 2)
    h_rows = pl.ds(pl.multiple_of(h * half, half), half)
    o_rows = pl.ds(pl.multiple_of((1 - h) * half, half), half)

    def piece(i):
        chip = lax.rem(z + parity + 2 * i, n)
        block = b_in.at[chip // 2]
        same = remote(block.at[h_rows], b_all.at[z, h], b_send.at[i, 0], b_recv.at[z], dp=chip, mp=h)
        other = remote(
            block.at[o_rows], b_all.at[z, 1 - h], b_send.at[i, 1], b_recv.at[z], dp=chip, mp=1 - h
        )
        return same, other

    self_chip = parity == 0
    self_copy = pltpu.make_async_copy(
        b_in.at[z // 2].at[h_rows], b_all.at[z, h], b_recv.at[z]
    )
    order = []
    for i in range(n // 4):
        order.extend([i, n // 2 - 1 - i])
    for i in order:
        same, other = piece(i)
        if i == 0:
            @pl.when(self_chip)
            def _():
                self_copy.start()

            @pl.when(jnp.logical_not(self_chip))
            def _():
                same.start()
        else:
            same.start()
        other.start()

    def forward(at):
        got = remote(b_all.at[at, h], b_all.at[at, h], b_send.at[0, 0], b_recv.at[at], mp=1 - h)
        got.wait_recv()
        out = remote(b_all.at[at, h], b_all.at[at, h], f_send.at[at], f_recv.at[at], mp=1 - h)
        out.start()

    forward(z)
    for step in range(steps):
        ring_recv(step)
        if step < steps - 1:
            ring_send(step + 1)
        if step == steps - 1:
            forward(lax.rem(z + steps, n))
        else:
            forward(lax.rem(z + step + 1, n))
            forward(lax.rem(z + n - step - 1, n))
    for o in range(n):
        at = lax.rem(z + o, n)
        end = remote(
            b_all.at[at, 1 - h], b_all.at[at, 1 - h], f_send.at[at], f_recv.at[at], mp=1 - h
        )
        end.wait_send()
        end.wait_recv()
    for one in right_sends + left_sends:
        one.wait_send()
    for i in range(n // 2):
        same, other = piece(i)
        if i == 0:
            @pl.when(jnp.logical_not(self_chip))
            def _():
                same.wait_send()
        else:
            same.wait_send()
        other.wait_send()
    own.wait()
    table.wait()


def collect(a_part, b_part, table, n):
    tok, width = a_part.shape
    cols = b_part.shape[2]
    dma = pltpu.SemaphoreType.DMA
    vmem = pl.BlockSpec(memory_space=pltpu.VMEM)
    return pl.pallas_call(
        functools.partial(collect_kernel, n),
        out_shape=(
            jax.ShapeDtypeStruct((n, tok, width), jnp.bfloat16),
            jax.ShapeDtypeStruct((n, 2, tok // 2, cols), jnp.bfloat16),
            jax.ShapeDtypeStruct(table.shape, jnp.int32),
        ),
        in_specs=[vmem] * 3,
        out_specs=(vmem,) * 3,
        scratch_shapes=[
            dma((n // 2,)), dma((n // 2,)), dma((n // 2,)), dma((n // 2,)),
            dma((n // 2, 2)), dma((n,)), dma((n,)), dma((n,)), dma(()), dma(()), dma(()),
        ],
        compiler_params=pltpu.CompilerParams(collective_id=1, has_side_effects=True),
        name="collect",
    )(a_part, b_part, table)


def home_of(block, blocks, n):
    return (n * block) // blocks


def to_home_kernel(n, rows, cols, g_in, out, send, recv):
    z = lax.axis_index("dp")
    h = lax.axis_index("mp")
    blocks = rows * cols
    half = BLK // 2
    greet_group(n, z, h)
    m = lax.rem(z, 2)
    j = z // 2
    source = z * 2 + h
    dst = out.at[pl.ds(pl.multiple_of(h * half, half), half), pl.ds(pl.multiple_of(j * LANE, LANE), LANE)]
    moves = []
    for block in range(blocks):
        row, col = block // cols, block % cols
        home = lax.rem(home_of(block, blocks, n) + SHIFT * m, n)
        src = g_in.at[pl.ds(row * half, half), pl.ds(col * LANE, LANE)]
        mine = jnp.logical_and(home == z, h == m)
        moves.append((
            mine,
            pltpu.make_async_copy(src, dst, recv.at[source]),
            remote(src, dst, send.at[block], recv.at[source], dp=home, mp=m),
        ))
    for mine, local, far in moves:
        @pl.when(mine)
        def _():
            local.start()

        @pl.when(jnp.logical_not(mine))
        def _():
            far.start()

    spot = lax.rem(z + n - SHIFT * h, n)
    busy = functools.reduce(
        jnp.logical_or, [spot == home_of(block, blocks, n) for block in range(blocks)]
    )

    @pl.when(busy)
    def _():
        for jj in range(n // 2):
            for t in range(2):
                sem = recv.at[(2 * jj + h) * 2 + t]
                part = out.at[pl.ds(t * half, half), pl.ds(jj * LANE, LANE)]
                pltpu.make_async_copy(part, part, sem).wait()

    @pl.when(jnp.logical_not(busy))
    def _():
        out[...] = jnp.zeros_like(out)

    for mine, local, far in moves:
        @pl.when(jnp.logical_not(mine))
        def _():
            far.wait_send()


def to_home(shard, n, rows, cols):
    dma = pltpu.SemaphoreType.DMA
    vmem = pl.BlockSpec(memory_space=pltpu.VMEM)
    return pl.pallas_call(
        functools.partial(to_home_kernel, n, rows, cols),
        out_shape=jax.ShapeDtypeStruct((BLK, BLK), jnp.bfloat16),
        in_specs=[vmem],
        out_specs=vmem,
        scratch_shapes=[dma((rows * cols,)), dma((2 * n,))],
        compiler_params=pltpu.CompilerParams(collective_id=2, has_side_effects=True),
        name="to_home",
    )(shard)


PIECES = 8
KEEP = 5
BUSY_AT = (0, 1, 3, 4, 6)
IDLE_AT = (2, 5, 7)
MOVES = {
    0: ((5, -1, 2), (6, -1, 3), (7, -1, 4)),
    1: ((5, 1, 0), (6, 1, 1), (7, 1, 2)),
    3: ((5, -1, 3), (6, -1, 4), (7, 2, 0)),
    4: ((5, 1, 1), (6, 1, 2), (7, 1, 3)),
    6: ((5, -1, 4), (6, 1, 0), (7, 1, 1)),
}


def spread_kernel(n, upd, out, send, recv, loc):
    z = lax.axis_index("dp")
    h = lax.axis_index("mp")
    greet_group(n, z, h)
    spot = lax.rem(lax.rem(z + n - SHIFT * h, n), 8)
    high = BLK // PIECES
    for at in BUSY_AT:
        @pl.when(spot == at)
        def _(at=at):
            sends = []
            for index, (part, step, slot) in enumerate(MOVES[at]):
                go = remote(
                    upd.at[pl.ds(part * high, high)], out.at[slot], send.at[index], recv.at[slot],
                    dp=lax.rem(z + n + step, n),
                )
                go.start()
                sends.append(go)
            for part in range(KEEP):
                out[part] = upd[pl.ds(part * high, high), :]
            for go in sends:
                go.wait_send()

    idle = functools.reduce(jnp.logical_or, [spot == at for at in IDLE_AT])

    @pl.when(idle)
    def _():
        for slot in range(KEEP):
            pltpu.make_async_copy(out.at[slot], out.at[slot], recv.at[slot]).wait()


def spread(upd, n):
    dma = pltpu.SemaphoreType.DMA
    vmem = pl.BlockSpec(memory_space=pltpu.VMEM)
    return pl.pallas_call(
        functools.partial(spread_kernel, n),
        out_shape=jax.ShapeDtypeStruct((KEEP, BLK // PIECES, BLK), jnp.bfloat16),
        in_specs=[vmem],
        out_specs=vmem,
        scratch_shapes=[dma((3,)), dma((KEEP,)), dma(())],
        compiler_params=pltpu.CompilerParams(collective_id=3, has_side_effects=True),
        name="spread",
    )(upd)


def piece_tables(n, rows, cols):
    blocks = rows * cols
    device = np.zeros((rows, PIECES, cols), np.int32)
    slot = np.zeros((rows, PIECES, cols), np.int32)
    for block in range(blocks):
        home = home_of(block, blocks, n)
        row, col = block // cols, block % cols
        for part in range(KEEP):
            device[row, part, col] = home
            slot[row, part, col] = part
        for part, step, at in MOVES[home % 8]:
            device[row, part, col] = (home + step) % n
            slot[row, part, col] = at
    return device, slot


def place_kernel(cols, table, *refs):
    scale_ref, out = refs[cols], refs[cols + 1]
    scale = scale_ref[0]
    for col in range(cols):
        wide = refs[col][0].astype(jnp.float32)
        out[:, col * BLK:(col + 1) * BLK] = (wide * scale).astype(jnp.bfloat16)


def place(gathered, table, scale, rows, cols):
    high = BLK // PIECES
    picks = [
        pl.BlockSpec((1, high, BLK), lambda g, tab, col=col: (tab[g * cols + col], 0, 0))
        for col in range(cols)
    ]
    return pl.pallas_call(
        functools.partial(place_kernel, cols),
        out_shape=jax.ShapeDtypeStruct((rows * BLK, cols * BLK), jnp.bfloat16),
        grid_spec=pltpu.PrefetchScalarGridSpec(
            num_scalar_prefetch=1,
            grid=(rows * PIECES,),
            in_specs=picks + [pl.BlockSpec(memory_space=pltpu.SMEM)],
            out_specs=pl.BlockSpec((high, cols * BLK), lambda g, tab: (g, 0)),
        ),
        name="place",
    )(table, *([gathered] * cols), scale)


def on_device(activations, out_grads, slot_table, exponent_index, damping_index):
    n = lax.axis_size("dp")
    z = lax.axis_index("dp")
    h = lax.axis_index("mp")
    tok = activations.shape[0]
    rows = activations.shape[1] // BLK
    cols = out_grads.shape[1] // BLK
    blocks = rows * cols
    half = BLK // 2
    pieces = BLK // LANE

    act = activations.reshape(tok, rows, 2, half)
    act = jnp.where(h == 0, act[:, :, 0], act[:, :, 1]).reshape(tok, rows * half)
    grads = out_grads.reshape(tok, cols, pieces, LANE).transpose(2, 0, 1, 3)
    grads = grads.reshape(pieces, tok, cols * LANE)
    table_row = jnp.broadcast_to(
        jnp.pad(slot_table, ((0, 0), (0, LANE - n))), (8, LANE)
    ).astype(jnp.int32)
    a_all, b_all, other_table = collect(act, grads, table_row, n)

    shard = lax.dot_general(
        a_all.reshape(n * tok, rows * half), b_all.reshape(n * tok, cols * LANE),
        (((0,), (0,)), ((), ())), preferred_element_type=jnp.float32,
    ).astype(jnp.bfloat16)

    home_grad = to_home(shard, n, rows, cols)

    shard_after, home_grad = lax.optimization_barrier((shard, home_grad))
    served = jnp.where(lax.rem(z, 2) == h, slot_table[0], other_table[0, :n])[:blocks]
    hits = served[None, :] == jnp.arange(n, dtype=jnp.int32)[:, None]
    filled = jnp.any(hits, axis=1)
    picks = jnp.sum(jnp.where(hits, jnp.arange(blocks, dtype=jnp.int32)[None, :], 0), axis=1)
    by_block = shard_after.reshape(rows, half, cols, LANE).transpose(0, 2, 1, 3)
    by_block = by_block.reshape(blocks, half, LANE)
    payload = jnp.where(filled[:, None, None], jnp.take(by_block, picks, axis=0), jnp.zeros((), jnp.bfloat16))
    arrived = lax.all_to_all(payload, "dp", split_axis=0, concat_axis=0, tiled=True)

    spot = lax.rem(z + n - SHIFT * h, n)
    homes = jnp.asarray([home_of(b, blocks, n) for b in range(blocks)], jnp.int32)
    block_here = jnp.sum(jnp.where(homes == spot, jnp.arange(blocks, dtype=jnp.int32), 0))
    slot_here = jnp.sum(jnp.where(jnp.arange(n) == block_here, slot_table[0], 0))
    at_slot = jnp.arange(n, dtype=jnp.int32) == slot_here
    exp_here = jnp.sum(jnp.where(at_slot, exponent_index[0], 0))
    damp_here = jnp.sum(jnp.where(at_slot, damping_index[0], 0))
    left_root, right_root = two_roots(home_grad, exp_here, damp_here)
    half_step = jnp.dot(left_root, home_grad, preferred_element_type=jnp.float32).astype(jnp.bfloat16)
    block_update = jnp.dot(half_step, right_root, preferred_element_type=jnp.float32).astype(jnp.bfloat16)
    dense = spread(block_update, n)
    gathered = lax.all_gather(dense, "dp", axis=0, tiled=True)

    wide = dense.astype(jnp.float32)
    total_sq = lax.psum(jnp.sum(wide * wide), ("dp", "mp"))
    entries = rows * BLK * cols * BLK * lax.axis_size("mp")
    rescale = lax.rsqrt(total_sq / entries + 1.0)

    swap = arrived.reshape(n // 2, 2, half, LANE).transpose(1, 0, 2, 3)
    swap = lax.all_to_all(swap, "mp", split_axis=0, concat_axis=0, tiled=True)
    slot_grad = swap.transpose(0, 2, 1, 3).reshape(BLK, BLK)
    at_own = jnp.arange(n, dtype=jnp.int32) == z
    exp_own = jnp.sum(jnp.where(at_own, exponent_index[0], 0))
    damp_own = jnp.sum(jnp.where(at_own, damping_index[0], 0))
    roots = jnp.stack(two_roots(slot_grad, exp_own, damp_own))

    device_tab, slot_tab = piece_tables(n, rows, cols)
    table = lax.rem(jnp.asarray(device_tab) + SHIFT * h, n) * KEEP + jnp.asarray(slot_tab)
    update = place(gathered, table.reshape(-1), rescale.reshape(1), rows, cols)
    return (update, roots[None, None])


def solution(mesh):
    placed = (
        P(("member", "dp"), None),
        P(("member", "dp"), "mp"),
        P(("member", "mp"), None),
        P(("member", "mp"), None),
        P(("member", "mp"), None),
    )
    return jax.shard_map(
        on_device,
        mesh=mesh,
        in_specs=placed,
        out_specs=(P("member", "mp"), P(("member", "mp"), "dp", None, None, None)),
        check_vma=False,
    )
```

```python
import functools

import jax
import jax.numpy as jnp
import numpy as np
from jax import lax
from jax.experimental import pallas as pl
from jax.experimental.pallas import tpu as pltpu
from jax.sharding import PartitionSpec as P


BLK = 1024
LANE = 128
ROOT_ORDERS = (2.0, 4.0)
DAMPINGS = (0.03, 0.1, 0.3, 1.0)
SHIFT = 4
MESH = pl.DeviceIdType.MESH


def table_value(picked, values_table):
    values = jnp.asarray(values_table, jnp.float32)
    matches = jnp.arange(len(values_table), dtype=jnp.int32) == picked
    return jnp.sum(jnp.where(matches, values, 0.0))


def half_dot(first, second):
    return jnp.dot(
        first.astype(jnp.bfloat16), second.astype(jnp.bfloat16), preferred_element_type=jnp.float32
    )


def inverse_root(statistic, root_order, quartic, damping):
    dimension = statistic.shape[0]
    identity = jnp.eye(dimension, dtype=jnp.float32)
    damped = statistic + damping * (jnp.trace(statistic) / dimension + 1.0) * identity
    current = damped * (dimension / (2.0 * jnp.trace(damped)))
    factor = ((root_order + 1.0) * identity - current) / root_order
    estimate = factor
    square = half_dot(factor, factor)
    fourth = half_dot(square, square)
    raised = jnp.where(quartic, fourth, square)
    current = half_dot(raised, current)
    factor = ((root_order + 1.0) * identity - current) / root_order
    estimate = half_dot(estimate, factor)
    return estimate.astype(jnp.bfloat16)


def two_roots(gradient, exp_pick, damp_pick):
    root_order = table_value(exp_pick, ROOT_ORDERS)
    quartic = exp_pick == 1
    damping = table_value(damp_pick, DAMPINGS)
    left_stat = lax.dot_general(
        gradient, gradient, (((1,), (1,)), ((), ())), preferred_element_type=jnp.float32
    )
    right_stat = lax.dot_general(
        gradient, gradient, (((0,), (0,)), ((), ())), preferred_element_type=jnp.float32
    )
    return (
        inverse_root(left_stat, root_order, quartic, damping),
        inverse_root(right_stat, root_order, quartic, damping),
    )


def greet_group(n, z, h):
    barrier = pltpu.get_barrier_semaphore()
    pl.semaphore_signal(barrier, inc=1, device_id={"mp": 1 - h}, device_id_type=MESH)
    for o in range(1, n):
        for t in range(2):
            pl.semaphore_signal(
                barrier, inc=1, device_id={"dp": lax.rem(z + o, n), "mp": t}, device_id_type=MESH
            )
    pl.semaphore_wait(barrier, 2 * n - 1)


def remote(src, dst, send, recv, **to):
    return pltpu.make_async_remote_copy(
        src_ref=src, dst_ref=dst, send_sem=send, recv_sem=recv, device_id=to, device_id_type=MESH
    )


def collect_kernel(
    n, a_in, b_in, tbl_in, a_all, b_all, tbl_out,
    as_r, ar_r, as_l, ar_l, b_send, b_recv, f_send, f_recv, t_send, t_recv, loc_sem,
):
    z = lax.axis_index("dp")
    h = lax.axis_index("mp")
    tok = a_in.shape[0]
    half = tok // 2
    right, left = lax.rem(z + 1, n), lax.rem(z + n - 1, n)
    greet_group(n, z, h)
    steps = n // 2
    top, low = pl.ds(0, half), pl.ds(half, half)
    right_sends = []
    left_sends = []

    def ring_send(step):
        if step == 0:
            src_r = src_l = a_in
            at_r = at_l = z
        else:
            at_r = lax.rem(z + n - step, n)
            at_l = lax.rem(z + step, n)
            src_r, src_l = a_all.at[at_r], a_all.at[at_l]
        dst_r, dst_l = a_all.at[at_r], a_all.at[at_l]
        if step == steps - 1:
            src_r, dst_r = src_r.at[top], dst_r.at[top]
            src_l, dst_l = src_l.at[low], dst_l.at[low]
        one = remote(src_r, dst_r, as_r.at[step], ar_r.at[step], dp=right)
        two = remote(src_l, dst_l, as_l.at[step], ar_l.at[step], dp=left)
        one.start()
        two.start()
        right_sends.append(one)
        left_sends.append(two)

    def ring_recv(step):
        at_r = lax.rem(z + n - step - 1, n)
        at_l = lax.rem(z + step + 1, n)
        dst_r, dst_l = a_all.at[at_r], a_all.at[at_l]
        if step == steps - 1:
            dst_r, dst_l = dst_r.at[top], dst_l.at[low]
        remote(dst_r, dst_r, as_r.at[step], ar_r.at[step], dp=right).wait_recv()
        remote(dst_l, dst_l, as_l.at[step], ar_l.at[step], dp=left).wait_recv()

    table = remote(tbl_in, tbl_out, t_send, t_recv, mp=1 - h)
    table.start()
    own = pltpu.make_async_copy(a_in, a_all.at[z], loc_sem)
    own.start()
    ring_send(0)
    parity = lax.rem(z + h, 2)
    h_rows = pl.ds(pl.multiple_of(h * half, half), half)
    o_rows = pl.ds(pl.multiple_of((1 - h) * half, half), half)

    def piece(i):
        chip = lax.rem(z + parity + 2 * i, n)
        block = b_in.at[chip // 2]
        same = remote(block.at[h_rows], b_all.at[z, h], b_send.at[i, 0], b_recv.at[z], dp=chip, mp=h)
        other = remote(
            block.at[o_rows], b_all.at[z, 1 - h], b_send.at[i, 1], b_recv.at[z], dp=chip, mp=1 - h
        )
        return same, other

    self_chip = parity == 0
    self_copy = pltpu.make_async_copy(
        b_in.at[z // 2].at[h_rows], b_all.at[z, h], b_recv.at[z]
    )
    order = []
    for i in range(n // 4):
        order.extend([i, n // 2 - 1 - i])
    for i in order:
        same, other = piece(i)
        if i == 0:
            @pl.when(self_chip)
            def _():
                self_copy.start()

            @pl.when(jnp.logical_not(self_chip))
            def _():
                same.start()
        else:
            same.start()
        other.start()

    def forward(at):
        got = remote(b_all.at[at, h], b_all.at[at, h], b_send.at[0, 0], b_recv.at[at], mp=1 - h)
        got.wait_recv()
        out = remote(b_all.at[at, h], b_all.at[at, h], f_send.at[at], f_recv.at[at], mp=1 - h)
        out.start()

    forward(z)
    for step in range(steps):
        ring_recv(step)
        if step < steps - 1:
            ring_send(step + 1)
        if step == steps - 1:
            forward(lax.rem(z + steps, n))
        else:
            forward(lax.rem(z + step + 1, n))
            forward(lax.rem(z + n - step - 1, n))
    for o in range(n):
        at = lax.rem(z + o, n)
        end = remote(
            b_all.at[at, 1 - h], b_all.at[at, 1 - h], f_send.at[at], f_recv.at[at], mp=1 - h
        )
        end.wait_send()
        end.wait_recv()
    for one in right_sends + left_sends:
        one.wait_send()
    for i in range(n // 2):
        same, other = piece(i)
        if i == 0:
            @pl.when(jnp.logical_not(self_chip))
            def _():
                same.wait_send()
        else:
            same.wait_send()
        other.wait_send()
    own.wait()
    table.wait()


def collect(a_part, b_part, table, n):
    tok, width = a_part.shape
    cols = b_part.shape[2]
    dma = pltpu.SemaphoreType.DMA
    vmem = pl.BlockSpec(memory_space=pltpu.VMEM)
    return pl.pallas_call(
        functools.partial(collect_kernel, n),
        out_shape=(
            jax.ShapeDtypeStruct((n, tok, width), jnp.bfloat16),
            jax.ShapeDtypeStruct((n, 2, tok // 2, cols), jnp.bfloat16),
            jax.ShapeDtypeStruct(table.shape, jnp.int32),
        ),
        in_specs=[vmem] * 3,
        out_specs=(vmem,) * 3,
        scratch_shapes=[
            dma((n // 2,)), dma((n // 2,)), dma((n // 2,)), dma((n // 2,)),
            dma((n // 2, 2)), dma((n,)), dma((n,)), dma((n,)), dma(()), dma(()), dma(()),
        ],
        compiler_params=pltpu.CompilerParams(collective_id=1, has_side_effects=True),
        name="collect",
    )(a_part, b_part, table)


def home_of(block, blocks, n):
    return (n * block) // blocks


def to_home_kernel(n, rows, cols, g_in, out, send, recv):
    z = lax.axis_index("dp")
    h = lax.axis_index("mp")
    blocks = rows * cols
    half = BLK // 2
    greet_group(n, z, h)
    m = lax.rem(z, 2)
    j = z // 2
    source = z * 2 + h
    dst = out.at[pl.ds(pl.multiple_of(h * half, half), half), pl.ds(pl.multiple_of(j * LANE, LANE), LANE)]

    def moves(o):
        chip = lax.rem(z + o, n)
        at = lax.rem(chip + n - SHIFT * m, n)
        block = (at * blocks + n - 1) // n
        used = jnp.logical_and(block < blocks, (n * block) // blocks == at)
        src = g_in.at[
            pl.ds(pl.multiple_of((block // cols) * half, half), half),
            pl.ds(pl.multiple_of(lax.rem(block, cols) * LANE, LANE), LANE),
        ]
        local = pltpu.make_async_copy(src, dst, recv.at[source])
        far = remote(src, dst, send.at[o], recv.at[source], dp=chip, mp=m)
        mine = h == m if o == 0 else False
        return used, mine, local, far

    order = [n // 2]
    for o in range(n // 2 - 1, 0, -1):
        order.extend([o, n - o])
    for o in order + [0]:
        used, mine, local, far = moves(o)
        if o == 0:
            @pl.when(jnp.logical_and(used, mine))
            def _():
                local.start()

            used = jnp.logical_and(used, jnp.logical_not(mine))

        @pl.when(used)
        def _():
            far.start()

    spot = lax.rem(z + n - SHIFT * h, n)
    busy = functools.reduce(
        jnp.logical_or, [spot == home_of(block, blocks, n) for block in range(blocks)]
    )

    @pl.when(busy)
    def _():
        for jj in range(n // 2):
            for t in range(2):
                sem = recv.at[(2 * jj + h) * 2 + t]
                part = out.at[pl.ds(t * half, half), pl.ds(jj * LANE, LANE)]
                pltpu.make_async_copy(part, part, sem).wait()

    @pl.when(jnp.logical_not(busy))
    def _():
        out[...] = jnp.zeros_like(out)

    for o in range(n):
        used, mine, local, far = moves(o)
        if o == 0:
            used = jnp.logical_and(used, jnp.logical_not(mine))

        @pl.when(used)
        def _():
            far.wait_send()


def to_home(shard, n, rows, cols):
    dma = pltpu.SemaphoreType.DMA
    vmem = pl.BlockSpec(memory_space=pltpu.VMEM)
    return pl.pallas_call(
        functools.partial(to_home_kernel, n, rows, cols),
        out_shape=jax.ShapeDtypeStruct((BLK, BLK), jnp.bfloat16),
        in_specs=[vmem],
        out_specs=vmem,
        scratch_shapes=[dma((n,)), dma((2 * n,))],
        compiler_params=pltpu.CompilerParams(collective_id=2, has_side_effects=True),
        name="to_home",
    )(shard)


PIECES = 8
KEEP = 5
BUSY_AT = (0, 1, 3, 4, 6)
IDLE_AT = (2, 5, 7)
MOVES = {
    0: ((5, -1, 2), (6, -1, 3), (7, -1, 4)),
    1: ((5, 1, 0), (6, 1, 1), (7, 1, 2)),
    3: ((5, -1, 3), (7, -1, 4), (6, 2, 0)),
    4: ((5, 1, 1), (6, 1, 2), (7, 1, 3)),
    6: ((7, -1, 4), (5, 1, 0), (6, 1, 1)),
}


def spread_kernel(n, upd, out, send, recv, loc):
    z = lax.axis_index("dp")
    h = lax.axis_index("mp")
    greet_group(n, z, h)
    spot = lax.rem(lax.rem(z + n - SHIFT * h, n), 8)
    high = BLK // PIECES
    for at in BUSY_AT:
        @pl.when(spot == at)
        def _(at=at):
            sends = []
            for index, (part, step, slot) in enumerate(MOVES[at]):
                go = remote(
                    upd.at[pl.ds(part * high, high)], out.at[slot], send.at[index], recv.at[slot],
                    dp=lax.rem(z + n + step, n),
                )
                go.start()
                sends.append(go)
            for part in range(KEEP):
                out[part] = upd[pl.ds(part * high, high), :]
            for go in sends:
                go.wait_send()

    idle = functools.reduce(jnp.logical_or, [spot == at for at in IDLE_AT])

    @pl.when(idle)
    def _():
        for slot in range(KEEP):
            pltpu.make_async_copy(out.at[slot], out.at[slot], recv.at[slot]).wait()


def spread(upd, n):
    dma = pltpu.SemaphoreType.DMA
    vmem = pl.BlockSpec(memory_space=pltpu.VMEM)
    return pl.pallas_call(
        functools.partial(spread_kernel, n),
        out_shape=jax.ShapeDtypeStruct((KEEP, BLK // PIECES, BLK), jnp.bfloat16),
        in_specs=[vmem],
        out_specs=vmem,
        scratch_shapes=[dma((3,)), dma((KEEP,)), dma(())],
        compiler_params=pltpu.CompilerParams(collective_id=3, has_side_effects=True),
        name="spread",
    )(upd)


def piece_tables(n, rows, cols):
    blocks = rows * cols
    device = np.zeros((rows, PIECES, cols), np.int32)
    slot = np.zeros((rows, PIECES, cols), np.int32)
    for block in range(blocks):
        home = home_of(block, blocks, n)
        row, col = block // cols, block % cols
        for part in range(KEEP):
            device[row, part, col] = home
            slot[row, part, col] = part
        for part, step, at in MOVES[home % 8]:
            device[row, part, col] = (home + step) % n
            slot[row, part, col] = at
    return device, slot


def place_early_kernel(cols, table, groups, *refs):
    scale_ref, out = refs[cols], refs[-1]
    scale = scale_ref[0]
    for col in range(cols):
        wide = refs[col][0].astype(jnp.float32)
        out[:, col * BLK:(col + 1) * BLK] = (wide * scale).astype(jnp.bfloat16)


def place_late_kernel(cols, early, late, choice, groups, *refs):
    scale_ref, out = refs[2 * cols], refs[-1]
    scale = scale_ref[0]
    g = pl.program_id(0)
    for col in range(cols):
        for kind in range(2):
            @pl.when(choice[g * cols + col] == kind)
            def _(col=col, kind=kind):
                wide = refs[kind * cols + col][0].astype(jnp.float32)
                out[:, col * BLK:(col + 1) * BLK] = (wide * scale).astype(jnp.bfloat16)


def place_early(gathered, table, groups, scale, rows, cols):
    high = BLK // PIECES
    picks = [
        pl.BlockSpec((1, high, BLK), lambda g, tab, grp, col=col: (tab[g * cols + col], 0, 0))
        for col in range(cols)
    ]
    return pl.pallas_call(
        functools.partial(place_early_kernel, cols),
        out_shape=jax.ShapeDtypeStruct((rows * BLK, cols * BLK), jnp.bfloat16),
        grid_spec=pltpu.PrefetchScalarGridSpec(
            num_scalar_prefetch=2,
            grid=(groups.shape[0],),
            in_specs=picks + [pl.BlockSpec(memory_space=pltpu.SMEM)],
            out_specs=pl.BlockSpec((high, cols * BLK), lambda g, tab, grp: (grp[g], 0)),
        ),
        cost_estimate=pl.CostEstimate(
            flops=int(2e9), bytes_accessed=int(3e7), transcendentals=0
        ),
        name="place_early",
    )(table, groups, *([gathered] * cols), scale)


def place_late(gathered_early, gathered_late, early, late, choice, groups, scale, before, rows, cols):
    high = BLK // PIECES
    picks = [
        pl.BlockSpec((1, high, BLK), lambda g, ta, tb, ch, grp, col=col: (ta[g * cols + col], 0, 0))
        for col in range(cols)
    ] + [
        pl.BlockSpec((1, high, BLK), lambda g, ta, tb, ch, grp, col=col: (tb[g * cols + col], 0, 0))
        for col in range(cols)
    ]
    return pl.pallas_call(
        functools.partial(place_late_kernel, cols),
        out_shape=jax.ShapeDtypeStruct((rows * BLK, cols * BLK), jnp.bfloat16),
        grid_spec=pltpu.PrefetchScalarGridSpec(
            num_scalar_prefetch=4,
            grid=(groups.shape[0],),
            in_specs=picks
            + [pl.BlockSpec(memory_space=pltpu.SMEM), pl.BlockSpec(memory_space=pl.ANY)],
            out_specs=pl.BlockSpec((high, cols * BLK), lambda g, ta, tb, ch, grp: (grp[g], 0)),
        ),
        input_output_aliases={4 + 2 * cols + 1: 0},
        name="place_late",
    )(early, late, choice, groups, *([gathered_early] * cols), *([gathered_late] * cols), scale, before)


EARLY = (0, 1, 2, 3, 5, 6)
LATE = (4, 7)


def inner(activations, out_grads, slot_table, exponent_index, damping_index):
    n = lax.axis_size("dp")
    z = lax.axis_index("dp")
    h = lax.axis_index("mp")
    tok = activations.shape[0]
    rows = activations.shape[1] // BLK
    cols = out_grads.shape[1] // BLK
    blocks = rows * cols
    half = BLK // 2
    pieces = BLK // LANE

    act = activations.reshape(tok, rows, 2, half)
    act = jnp.where(h == 0, act[:, :, 0], act[:, :, 1]).reshape(tok, rows * half)
    grads = out_grads.reshape(tok, cols, pieces, LANE).transpose(2, 0, 1, 3)
    grads = grads.reshape(pieces, tok, cols * LANE)
    table_row = jnp.broadcast_to(
        jnp.pad(slot_table, ((0, 0), (0, LANE - n))), (8, LANE)
    ).astype(jnp.int32)
    a_all, b_all, other_table = collect(act, grads, table_row, n)

    shard = lax.dot_general(
        a_all.reshape(n * tok, rows * half), b_all.reshape(n * tok, cols * LANE),
        (((0,), (0,)), ((), ())), preferred_element_type=jnp.float32,
    ).astype(jnp.bfloat16)

    home_grad = to_home(shard, n, rows, cols)

    shard_after, home_grad = lax.optimization_barrier((shard, home_grad))
    served = jnp.where(lax.rem(z, 2) == h, slot_table[0], other_table[0, :n])[:blocks]
    hits = served[None, :] == jnp.arange(n, dtype=jnp.int32)[:, None]
    filled = jnp.any(hits, axis=1)
    picks = jnp.sum(jnp.where(hits, jnp.arange(blocks, dtype=jnp.int32)[None, :], 0), axis=1)
    by_block = shard_after.reshape(rows, half, cols, LANE).transpose(0, 2, 1, 3)
    by_block = by_block.reshape(blocks, half, LANE)
    payload = jnp.where(filled[:, None, None], jnp.take(by_block, picks, axis=0), jnp.zeros((), jnp.bfloat16))
    arrived = lax.all_to_all(payload, "dp", split_axis=0, concat_axis=0, tiled=True)

    spot = lax.rem(z + n - SHIFT * h, n)
    homes = jnp.asarray([home_of(b, blocks, n) for b in range(blocks)], jnp.int32)
    block_here = jnp.sum(jnp.where(homes == spot, jnp.arange(blocks, dtype=jnp.int32), 0))
    slot_here = jnp.sum(jnp.where(jnp.arange(n) == block_here, slot_table[0], 0))
    at_slot = jnp.arange(n, dtype=jnp.int32) == slot_here
    exp_here = jnp.sum(jnp.where(at_slot, exponent_index[0], 0))
    damp_here = jnp.sum(jnp.where(at_slot, damping_index[0], 0))
    left_root, right_root = two_roots(home_grad, exp_here, damp_here)
    half_step = jnp.dot(left_root, home_grad, preferred_element_type=jnp.float32).astype(jnp.bfloat16)
    block_update = jnp.dot(half_step, right_root, preferred_element_type=jnp.float32).astype(jnp.bfloat16)
    dense = spread(block_update, n)
    first = KEEP - 1
    gathered_early = lax.all_gather(dense[:first], "dp", axis=0, tiled=True)
    gathered_late = lax.all_gather(dense[first:], "dp", axis=0, tiled=True)

    wide = dense.astype(jnp.float32)
    total_sq = lax.psum(jnp.sum(wide * wide), ("dp", "mp"))
    entries = rows * BLK * cols * BLK * lax.axis_size("mp")
    rescale = lax.rsqrt(total_sq / entries + 1.0)

    swap = arrived.reshape(n // 2, 2, half, LANE).transpose(1, 0, 2, 3)
    swap = lax.all_to_all(swap, "mp", split_axis=0, concat_axis=0, tiled=True)
    slot_grad = swap.transpose(0, 2, 1, 3).reshape(BLK, BLK)
    at_own = jnp.arange(n, dtype=jnp.int32) == z
    exp_own = jnp.sum(jnp.where(at_own, exponent_index[0], 0))
    damp_own = jnp.sum(jnp.where(at_own, damping_index[0], 0))
    roots = jnp.stack(two_roots(slot_grad, exp_own, damp_own))

    device_tab, slot_tab = piece_tables(n, rows, cols)
    in_late = slot_tab == first

    def tables_of(parts):
        device_of = lax.rem(jnp.asarray(device_tab[:, parts].reshape(-1)) + SHIFT * h, n)
        late = in_late[:, parts].reshape(-1)
        early_at = jnp.where(late, 0, device_of * first + jnp.asarray(slot_tab[:, parts].reshape(-1)))
        return early_at, jnp.where(late, device_of, 0), jnp.asarray(late.astype(np.int32))

    def groups_of(parts):
        return jnp.asarray([r * PIECES + i for r in range(rows) for i in parts], jnp.int32)

    scale = rescale.reshape(1)
    update = place_early(
        gathered_early, tables_of(EARLY)[0], groups_of(EARLY), scale, rows, cols
    )
    update = place_late(
        gathered_early, gathered_late, *tables_of(LATE), groups_of(LATE), scale, update, rows, cols
    )
    return (update, roots[None, None])


def solution(mesh):
    placed = (
        P(("member", "dp"), None),
        P(("member", "dp"), "mp"),
        P(("member", "mp"), None),
        P(("member", "mp"), None),
        P(("member", "mp"), None),
    )
    return jax.shard_map(
        inner,
        mesh=mesh,
        in_specs=placed,
        out_specs=(P("member", "mp"), P(("member", "mp"), "dp", None, None, None)),
        check_vma=False,
    )
```

```python
import functools

import jax
import jax.numpy as jnp
import numpy as np
from jax import lax
from jax.experimental import pallas as pl
from jax.experimental.pallas import tpu as pltpu
from jax.sharding import PartitionSpec as P

BLK = 1024
LANE = 128
ROOT_ORDERS = (2.0, 4.0)
DAMPINGS = (0.03, 0.1, 0.3, 1.0)
SHIFT = 4
MESH = pl.DeviceIdType.MESH


STRIPE = 256


def eye_stripe(at, size):
    row = lax.broadcasted_iota(jnp.int32, (STRIPE, size), 0) + at
    col = lax.broadcasted_iota(jnp.int32, (STRIPE, size), 1)
    return row == col


def dot32(first, second, dims=((1,), (0,))):
    return lax.dot_general(first, second, (dims, ((), ())), preferred_element_type=jnp.float32)


def over_stripes(size, body):
    def step(index, carry):
        body(pl.multiple_of(index * STRIPE, STRIPE))
        return carry

    lax.fori_loop(0, size // STRIPE, step, 0)


def root_into(g, root, order, quartic, damping, trace, gt, m0, t0, q, r, only=None):
    size = g.shape[0]
    shift = damping * (trace / size + 1.0)
    ratio = size / (2.0 * (trace + shift * size))
    base = g if gt is None else gt

    def stat(at):
        rows = pl.ds(at, STRIPE)
        s = dot32(base[rows, :], base[...], ((1,), (1,)))
        on = eye_stripe(at, size)
        scaled = jnp.where(on, s + shift, s) * ratio
        m0[rows, :] = scaled.astype(jnp.bfloat16)
        t0[rows, :] = (jnp.where(on, (order + 1.0) - scaled, -scaled) / order).astype(jnp.bfloat16)

    def square(at):
        rows = pl.ds(at, STRIPE)
        q[rows, :] = dot32(t0[rows, :], t0[...]).astype(jnp.bfloat16)

    def fourth(at):
        rows = pl.ds(at, STRIPE)
        f = dot32(q[rows, :], q[...])
        r[rows, :] = jnp.where(quartic, f, q[rows, :].astype(jnp.float32)).astype(jnp.bfloat16)

    def factor(at):
        rows = pl.ds(at, STRIPE)
        m = dot32(r[rows, :], m0[...])
        on = eye_stripe(at, size)
        q[rows, :] = (jnp.where(on, (order + 1.0) - m, -m) / order).astype(jnp.bfloat16)

    def last(at):
        rows = pl.ds(at, STRIPE)
        root[rows, :] = dot32(t0[rows, :], q[...]).astype(jnp.bfloat16)

    for index, body in enumerate((stat, square, fourth, factor, last)):
        if only is None or only == index:
            over_stripes(size, body)


def trace_and_turn(g, gt, acc):
    size = g.shape[0]
    acc[...] = jnp.zeros_like(acc)

    def body(at):
        rows = pl.ds(at, STRIPE)
        part = g[rows, :]
        wide = part.astype(jnp.float32)
        acc[...] += jnp.sum((wide * wide).reshape(STRIPE // 8, 8, size), axis=0)
        gt[:, rows] = part.T

    over_stripes(size, body)
    return jnp.sum(acc[...])


def picks_of(codes):
    quartic = codes[0] == 1
    order = jnp.where(quartic, ROOT_ORDERS[1], ROOT_ORDERS[0])
    damping = jnp.float32(DAMPINGS[0])
    for index in range(1, len(DAMPINGS)):
        damping = jnp.where(codes[1] == index, jnp.float32(DAMPINGS[index]), damping)
    return quartic, order, damping


def greet_group(n, z, h):
    barrier = pltpu.get_barrier_semaphore()
    pl.semaphore_signal(barrier, inc=1, device_id={"mp": 1 - h}, device_id_type=MESH)
    for o in range(1, n):
        for t in range(2):
            pl.semaphore_signal(
                barrier, inc=1, device_id={"dp": lax.rem(z + o, n), "mp": t}, device_id_type=MESH
            )
    pl.semaphore_wait(barrier, 2 * n - 1)


def remote(src, dst, send, recv, **to):
    return pltpu.make_async_remote_copy(
        src_ref=src, dst_ref=dst, send_sem=send, recv_sem=recv, device_id=to, device_id_type=MESH
    )


def landed(ref, sem):
    pltpu.make_async_copy(ref, ref, sem).wait()


def both_ways(n):
    order = [n // 2]
    for o in range(n // 2 - 1, 0, -1):
        order.extend([o, n - o])
    return order + [0]


QUARTERS = 4


def step_kernel(
    n, rows, cols,
    codes, table_own, a_in, b_in, table_in,
    raw, roots, parts,
    a_all, b_all, table_far, table_smem, acc, shard, payload, home_g, slot_g, upd, part_out,
    gt, m0, t0, q, r, lane_acc,
    as_r, ar_r, as_l, ar_l, b_send, b_recv, f_send, f_recv, t_send, t_recv, loc,
    h_send, h_recv, s_send, s_recv, p_send, p_recv, gs_r, gr_r, gs_l, gr_l,
):
    z = lax.axis_index("dp")
    h = lax.axis_index("mp")
    blocks = rows * cols
    width, tok = a_in.shape
    half_tok = tok // 2
    half = BLK // 2
    right, left = lax.rem(z + 1, n), lax.rem(z + n - 1, n)
    steps = n // 2
    greet_group(n, z, h)

    top, low = pl.ds(0, width // 2), pl.ds(width // 2, width // 2)
    ring = []

    def ring_send(step):
        if step == 0:
            src_r = src_l = a_in
            at_r = at_l = z
        else:
            at_r = lax.rem(z + n - step, n)
            at_l = lax.rem(z + step, n)
            src_r, src_l = a_all.at[at_r], a_all.at[at_l]
        dst_r, dst_l = a_all.at[at_r], a_all.at[at_l]
        if step == steps - 1:
            src_r, dst_r = src_r.at[top], dst_r.at[top]
            src_l, dst_l = src_l.at[low], dst_l.at[low]
        one = remote(src_r, dst_r, as_r.at[step], ar_r.at[step], dp=right)
        two = remote(src_l, dst_l, as_l.at[step], ar_l.at[step], dp=left)
        one.start()
        two.start()
        ring.extend([one, two])

    def ring_recv(step):
        dst_r = a_all.at[lax.rem(z + n - step - 1, n)]
        dst_l = a_all.at[lax.rem(z + step + 1, n)]
        if step == steps - 1:
            dst_r, dst_l = dst_r.at[top], dst_l.at[low]
        landed(dst_r, ar_r.at[step])
        landed(dst_l, ar_l.at[step])

    table = remote(table_in, table_far, t_send, t_recv, mp=1 - h)
    table.start()
    own_a = pltpu.make_async_copy(a_in, a_all.at[z], loc.at[0])
    own_a.start()
    ring_send(0)
    parity = lax.rem(z + h, 2)
    h_rows = pl.ds(pl.multiple_of(h * half_tok, half_tok), half_tok)
    o_rows = pl.ds(pl.multiple_of((1 - h) * half_tok, half_tok), half_tok)

    def piece(i):
        chip = lax.rem(z + parity + 2 * i, n)
        block = b_in.at[chip // 2]
        same = remote(block.at[h_rows], b_all.at[z, h], b_send.at[i, 0], b_recv.at[z], dp=chip, mp=h)
        other = remote(
            block.at[o_rows], b_all.at[z, 1 - h], b_send.at[i, 1], b_recv.at[z], dp=chip, mp=1 - h
        )
        return same, other

    self_chip = parity == 0
    order = []
    for i in range(n // 4):
        order.extend([i, n // 2 - 1 - i])
    for i in order:
        same, other = piece(i)
        if i == 0:
            @pl.when(self_chip)
            def _():
                pltpu.make_async_copy(
                    b_in.at[z // 2].at[h_rows], b_all.at[z, h], b_recv.at[z]
                ).start()

            @pl.when(jnp.logical_not(self_chip))
            def _():
                same.start()
        else:
            same.start()
        other.start()

    def forward(at):
        landed(b_all.at[at, h], b_recv.at[at])
        remote(b_all.at[at, h], b_all.at[at, h], f_send.at[at], f_recv.at[at], mp=1 - h).start()

    def add_source(at, fresh=False):
        landed(b_all.at[at, 1 - h], f_recv.at[at])

        def body(low_row):
            span = pl.ds(low_row, STRIPE)
            got = dot32(a_all[at, span, :], b_all[at].reshape(tok, cols * LANE))
            if fresh:
                acc[span, :] = got
            else:
                acc[span, :] += got

        over_stripes(width, body)

    forward(z)
    own_a.wait()
    for step in range(steps):
        ring_recv(step)
        if step < steps - 1:
            ring_send(step + 1)
        if step == steps - 1:
            forward(lax.rem(z + steps, n))
        else:
            forward(lax.rem(z + step + 1, n))
            forward(lax.rem(z + n - step - 1, n))
        if step == 0:
            add_source(z, True)
        else:
            add_source(lax.rem(z + step, n))
            add_source(lax.rem(z + n - step, n))
    add_source(lax.rem(z + steps, n))
    for row in range(rows):
        for col in range(cols):
            shard[row * cols + col] = acc[
                row * half:(row + 1) * half, col * LANE:(col + 1) * LANE
            ].astype(jnp.bfloat16)

    m = lax.rem(z, 2)
    j = z // 2
    source = z * 2 + h
    spot_of = lambda chip, side: lax.rem(chip + n - SHIFT * side, n)
    my_rows = pl.ds(pl.multiple_of(h * half, half), half)
    my_cols = pl.ds(pl.multiple_of(j * LANE, LANE), LANE)

    def home_move(o):
        chip = lax.rem(z + o, n)
        at = spot_of(chip, m)
        block = (at * blocks + n - 1) // n
        used = jnp.logical_and(block < blocks, (n * block) // blocks == at)
        block = jnp.minimum(block, blocks - 1)
        dst = home_g.at[my_rows, my_cols]
        far = remote(shard.at[block], dst, h_send.at[o], h_recv.at[source], dp=chip, mp=m)
        return used, block, dst, far

    def home_go(o, start):
        used, block, dst, far = home_move(o)
        if o == 0:
            if start:
                @pl.when(jnp.logical_and(used, h == m))
                def _():
                    pltpu.make_async_copy(shard.at[block], dst, h_recv.at[source]).start()

            used = jnp.logical_and(used, h != m)

        @pl.when(used)
        def _():
            if start:
                far.start()
            else:
                far.wait_send()

    for o in both_ways(n):
        home_go(o, True)

    table.wait()
    to_smem = pltpu.make_async_copy(table_far, table_smem, loc.at[1])
    to_smem.start()
    to_smem.wait()

    def slot_move(o):
        chip = lax.rem(z + o, n)
        dst = slot_g.at[my_rows, my_cols]
        return chip, dst, remote(payload.at[chip], dst, s_send.at[o], s_recv.at[source], dp=chip, mp=m)

    for slot in range(n):
        pick = jnp.int32(0)
        filled = jnp.int32(0)
        for block in range(blocks):
            served = jnp.where(m == h, table_own[0, block], table_smem[0, block])
            pick = jnp.where(served == slot, block, pick)
            filled = jnp.where(served == slot, 1, filled)
        part = shard[pick]
        payload[slot] = jnp.where(filled == 1, part, jnp.zeros_like(part))
    for o in both_ways(n):
        chip, dst, far = slot_move(o)
        if o == 0:
            @pl.when(h == m)
            def _():
                pltpu.make_async_copy(payload.at[chip], dst, s_recv.at[source]).start()

            @pl.when(h != m)
            def _():
                far.start()
        else:
            far.start()

    spot = spot_of(z, h)
    own_block = (spot * blocks + n - 1) // n
    busy = jnp.logical_and(own_block < blocks, (n * own_block) // blocks == spot)
    lane_acc[...] = jnp.zeros_like(lane_acc)

    def all_pieces(ref, sems):
        for jj in range(n // 2):
            for t in range(2):
                landed(
                    ref.at[pl.ds(t * half, half), pl.ds(jj * LANE, LANE)],
                    sems.at[(2 * jj + h) * 2 + t],
                )

    def place_of(block, quarter):
        high = BLK // QUARTERS
        return raw.at[
            pl.ds(pl.multiple_of((block // cols) * BLK + quarter * high, high), high),
            pl.ds(pl.multiple_of(lax.rem(block, cols) * BLK, BLK), BLK),
        ]

    def quarter_of(quarter):
        high = BLK // QUARTERS
        return upd.at[pl.ds(quarter * high, high)]

    def own_moves(quarter):
        block = jnp.minimum(own_block, blocks - 1)
        src, dst = quarter_of(quarter), place_of(block, quarter)
        return (
            remote(src, dst, gs_r.at[block, quarter], gr_r.at[block, quarter], dp=right),
            remote(src, dst, gs_l.at[block, quarter], gr_l.at[block, quarter], dp=left),
            pltpu.make_async_copy(src, dst, loc.at[2 + quarter]),
        )

    @pl.when(busy)
    def _():
        all_pieces(home_g, h_recv)
        quartic, order_p, damping = picks_of([codes[0], codes[1]])
        trace = trace_and_turn(home_g, gt, lane_acc)
        root_into(home_g, roots.at[0], order_p, quartic, damping, trace, None, m0, t0, q, r)
        root_into(home_g, roots.at[1], order_p, quartic, damping, trace, gt, m0, t0, q, r)

        def halve(at):
            span = pl.ds(at, STRIPE)
            q[span, :] = dot32(roots[0, span, :], home_g[...]).astype(jnp.bfloat16)

        over_stripes(BLK, halve)
        lane_acc[...] = jnp.zeros_like(lane_acc)

        def finish(at):
            span = pl.ds(at, STRIPE)
            block = dot32(q[span, :], roots[1]).astype(jnp.bfloat16)
            upd[span, :] = block
            wide = block.astype(jnp.float32)
            lane_acc[...] += jnp.sum((wide * wide).reshape(STRIPE // 8, 8, BLK), axis=0)

        over_stripes(BLK, finish)
        for quarter in range(QUARTERS):
            for one in own_moves(quarter):
                one.start()

    tile = lane_acc[:, :LANE]
    for part in range(1, BLK // LANE):
        tile = tile + lane_acc[:, part * LANE:(part + 1) * LANE]
    part_out[...] = tile
    parts[source] = tile

    hop_right, hop_left = n // 2, n - 1 - n // 2

    def right_block(i):
        x = lax.rem(spot + n - 1, n)
        block = lax.rem(((x + 1) * blocks - 1) // n + blocks - i, blocks)
        return block, lax.rem(spot + n - (n * block) // blocks, n)

    def left_block(i):
        block = lax.rem(((spot + 1) * blocks - 1) // n + 1 + i, blocks)
        return block, lax.rem((n * block) // blocks + n - spot, n)

    def stream(i, quarter, side, phase):
        block, far = (right_block if side == 0 else left_block)(i)
        limit = hop_right if side == 0 else hop_left
        recv = (gr_r if side == 0 else gr_l).at[block, quarter]
        send = (gs_r if side == 0 else gs_l).at[block, quarter]
        ref = place_of(block, quarter)
        go = remote(ref, ref, send, recv, dp=right if side == 0 else left)
        if phase == 0:
            @pl.when(far < limit)
            def _():
                landed(ref, recv)
                go.start()
        elif phase == 1:
            @pl.when(far == limit)
            def _():
                landed(ref, recv)
        else:
            @pl.when(far < limit)
            def _():
                go.wait_send()

    slot_vals = {}

    def slot_first():
        all_pieces(slot_g, s_recv)
        slot_vals["picks"] = picks_of([codes[2], codes[3]])
        slot_vals["trace"] = trace_and_turn(slot_g, gt, lane_acc)

    def slot_unit(side, body):
        def run():
            quartic, order_p, damping = slot_vals["picks"]
            root_into(
                slot_g, roots.at[side], order_p, quartic, damping, slot_vals["trace"],
                None if side == 0 else gt, m0, t0, q, r, only=body,
            )
        return run

    units = [slot_first] + [slot_unit(side, body) for side in range(2) for body in range(5)]

    def part_move(o, t):
        return remote(
            part_out, parts.at[source], p_send.at[o, t], p_recv.at[source],
            dp=lax.rem(z + o, n), mp=t,
        )

    def part_each(act):
        remote_self = remote(
            part_out, parts.at[source], p_send.at[0, 0], p_recv.at[source], mp=1 - h
        )
        act(remote_self)
        for o in range(1, n):
            for t in range(2):
                act(part_move(o, t))

    most = (blocks + 1) // 2
    for i in range(most):
        for quarter in range(QUARTERS):
            stream(i, quarter, 0, 0)
            stream(i, quarter, 1, 0)
            if i == 0 and quarter == 0:
                part_each(lambda go: go.start())
            if i > 0 and units:
                units.pop(0)()
    for unit in units:
        unit()
    for i in range(most):
        for quarter in range(QUARTERS):
            stream(i, quarter, 0, 1)
            stream(i, quarter, 1, 1)

    for o in range(1, n):
        chip = lax.rem(z + o, n)
        for t in range(2):
            landed(parts.at[chip * 2 + t], p_recv.at[chip * 2 + t])
    landed(parts.at[z * 2 + 1 - h], p_recv.at[z * 2 + 1 - h])
    part_each(lambda go: go.wait_send())
    for one in ring:
        one.wait_send()
    for i in range(n // 2):
        same, other = piece(i)
        if i == 0:
            @pl.when(jnp.logical_not(self_chip))
            def _():
                same.wait_send()
        else:
            same.wait_send()
        other.wait_send()
    for o in range(n):
        at = lax.rem(z + o, n)
        remote(b_all.at[at, h], b_all.at[at, h], f_send.at[at], f_recv.at[at], mp=1 - h).wait_send()
        home_go(o, False)
        chip, dst, far = slot_move(o)
        if o == 0:
            @pl.when(h != m)
            def _():
                far.wait_send()
        else:
            far.wait_send()

    @pl.when(busy)
    def _():
        for quarter in range(QUARTERS):
            one, two, local = own_moves(quarter)
            one.wait_send()
            two.wait_send()
            local.wait()

    for i in range(most):
        for quarter in range(QUARTERS):
            stream(i, quarter, 0, 2)
            stream(i, quarter, 1, 2)


def run_step(codes, table_own, a_part, b_part, table, n, rows, cols):
    width, tok = a_part.shape
    dma = pltpu.SemaphoreType.DMA
    smem = pl.BlockSpec(memory_space=pltpu.SMEM)
    vmem = pl.BlockSpec(memory_space=pltpu.VMEM)
    blocks = rows * cols
    half = BLK // 2
    bf = lambda *shape: pltpu.VMEM(shape, jnp.bfloat16)
    steps = n // 2
    return pl.pallas_call(
        functools.partial(step_kernel, n, rows, cols),
        out_shape=(
            jax.ShapeDtypeStruct((rows * BLK, cols * BLK), jnp.bfloat16),
            jax.ShapeDtypeStruct((2, BLK, BLK), jnp.bfloat16),
            jax.ShapeDtypeStruct((2 * n, 8, LANE), jnp.float32),
        ),
        in_specs=[smem, smem, vmem, vmem, vmem],
        out_specs=(pl.BlockSpec(memory_space=pl.ANY), vmem, vmem),
        scratch_shapes=[
            bf(n, width, tok), bf(n, 2, tok // 2, cols * LANE),
            pltpu.VMEM((8, LANE), jnp.int32), pltpu.SMEM((8, LANE), jnp.int32),
            pltpu.VMEM((width, cols * LANE), jnp.float32),
            bf(blocks, half, LANE), bf(n, half, LANE), bf(BLK, BLK), bf(BLK, BLK), bf(BLK, BLK),
            pltpu.VMEM((8, LANE), jnp.float32),
            bf(BLK, BLK), bf(BLK, BLK), bf(BLK, BLK), bf(BLK, BLK), bf(BLK, BLK),
            pltpu.VMEM((8, BLK), jnp.float32),
            dma((steps,)), dma((steps,)), dma((steps,)), dma((steps,)),
            dma((steps, 2)), dma((n,)), dma((n,)), dma((n,)), dma(()), dma(()),
            dma((2 + QUARTERS,)),
            dma((n,)), dma((2 * n,)), dma((n,)), dma((2 * n,)), dma((n, 2)), dma((2 * n,)),
            dma((blocks, QUARTERS)), dma((blocks, QUARTERS)),
            dma((blocks, QUARTERS)), dma((blocks, QUARTERS)),
        ],
        compiler_params=pltpu.CompilerParams(
            collective_id=1, has_side_effects=True, vmem_limit_bytes=60 << 20
        ),
        name="shampoo_step",
    )(codes, table_own, a_part, b_part, table)


def on_device(activations, out_grads, slot_table, exponent_index, damping_index):
    n = lax.axis_size("dp")
    z = lax.axis_index("dp")
    h = lax.axis_index("mp")
    tok = activations.shape[0]
    rows = activations.shape[1] // BLK
    cols = out_grads.shape[1] // BLK
    blocks = rows * cols
    half = BLK // 2
    pieces = BLK // LANE

    act = activations.reshape(tok, rows, 2, half)
    act = jnp.where(h == 0, act[:, :, 0], act[:, :, 1]).reshape(tok, rows * half).T
    grads = out_grads.reshape(tok, cols, pieces, LANE).transpose(2, 0, 1, 3)
    grads = grads.reshape(pieces, tok, cols * LANE)
    table_row = jnp.broadcast_to(
        jnp.pad(slot_table, ((0, 0), (0, LANE - n))), (8, LANE)
    ).astype(jnp.int32)

    spot = lax.rem(z + n - SHIFT * h, n)
    homes = np.asarray([(n * b) // blocks for b in range(blocks)], np.int32)
    lanes = jnp.arange(n, dtype=jnp.int32)
    block_here = jnp.sum(jnp.where(homes == spot, np.arange(blocks, dtype=np.int32), 0))
    slot_here = jnp.sum(jnp.where(lanes == block_here, slot_table[0], 0))
    spots = jnp.stack([lanes == slot_here, lanes == z])
    exps = jnp.sum(jnp.where(spots, exponent_index, 0), axis=1)
    damps = jnp.sum(jnp.where(spots, damping_index, 0), axis=1)
    codes = jnp.stack([exps, damps], axis=1).reshape(4).astype(jnp.int32)

    raw, roots, parts = run_step(codes, slot_table, act, grads, table_row, n, rows, cols)
    total_sq = jnp.sum(parts)
    entries = rows * BLK * cols * BLK * lax.axis_size("mp")
    rescale = lax.rsqrt(total_sq / entries + 1.0)
    update = (raw.astype(jnp.float32) * rescale).astype(jnp.bfloat16)
    return (update, roots[None, None])


def solution(mesh):
    placed = (
        P(("member", "dp"), None),
        P(("member", "dp"), "mp"),
        P(("member", "mp"), None),
        P(("member", "mp"), None),
        P(("member", "mp"), None),
    )
    return jax.shard_map(
        on_device,
        mesh=mesh,
        in_specs=placed,
        out_specs=(P("member", "mp"), P(("member", "mp"), "dp", None, None, None)),
        check_vma=False,
    )
```

```python
import functools

import jax
import jax.numpy as jnp
import numpy as np
from jax import lax
from jax.experimental import pallas as pl
from jax.experimental.pallas import tpu as pltpu
from jax.sharding import PartitionSpec as P

BLK = 1024
LANE = 128
ROOT_ORDERS = (2.0, 4.0)
DAMPINGS = (0.03, 0.1, 0.3, 1.0)
SHIFT = 4
MESH = pl.DeviceIdType.MESH


STRIPE = 256


def eye_stripe(at, size):
    row = lax.broadcasted_iota(jnp.int32, (STRIPE, size), 0) + at
    col = lax.broadcasted_iota(jnp.int32, (STRIPE, size), 1)
    return row == col


def dot32(first, second, dims=((1,), (0,))):
    return lax.dot_general(first, second, (dims, ((), ())), preferred_element_type=jnp.float32)


def over_stripes(size, body):
    def step(index, carry):
        body(pl.multiple_of(index * STRIPE, STRIPE))
        return carry

    lax.fori_loop(0, size // STRIPE, step, 0)


def root_into(g, root, order, quartic, damping, trace, gt, m0, t0, q, r, only=None):
    size = g.shape[0]
    shift = damping * (trace / size + 1.0)
    ratio = size / (2.0 * (trace + shift * size))
    base = g if gt is None else gt

    def stat(at):
        rows = pl.ds(at, STRIPE)
        s = dot32(base[rows, :], base[...], ((1,), (1,)))
        on = eye_stripe(at, size)
        scaled = jnp.where(on, s + shift, s) * ratio
        m0[rows, :] = scaled.astype(jnp.bfloat16)
        t0[rows, :] = (jnp.where(on, (order + 1.0) - scaled, -scaled) / order).astype(jnp.bfloat16)

    def square(at):
        rows = pl.ds(at, STRIPE)
        q[rows, :] = dot32(t0[rows, :], t0[...]).astype(jnp.bfloat16)

    def fourth(at):
        rows = pl.ds(at, STRIPE)
        f = dot32(q[rows, :], q[...])
        r[rows, :] = jnp.where(quartic, f, q[rows, :].astype(jnp.float32)).astype(jnp.bfloat16)

    def factor(at):
        rows = pl.ds(at, STRIPE)
        m = dot32(r[rows, :], m0[...])
        on = eye_stripe(at, size)
        q[rows, :] = (jnp.where(on, (order + 1.0) - m, -m) / order).astype(jnp.bfloat16)

    def last(at):
        rows = pl.ds(at, STRIPE)
        root[rows, :] = dot32(t0[rows, :], q[...]).astype(jnp.bfloat16)

    for index, body in enumerate((stat, square, fourth, factor, last)):
        if only is None or only == index:
            over_stripes(size, body)


def trace_and_turn(g, gt, acc):
    size = g.shape[0]
    acc[...] = jnp.zeros_like(acc)

    def body(at):
        rows = pl.ds(at, STRIPE)
        part = g[rows, :]
        wide = part.astype(jnp.float32)
        acc[...] += jnp.sum((wide * wide).reshape(STRIPE // 8, 8, size), axis=0)
        gt[:, rows] = part.T

    over_stripes(size, body)
    return jnp.sum(acc[...])


def picks_of(codes):
    quartic = codes[0] == 1
    order = jnp.where(quartic, ROOT_ORDERS[1], ROOT_ORDERS[0])
    damping = jnp.float32(DAMPINGS[0])
    for index in range(1, len(DAMPINGS)):
        damping = jnp.where(codes[1] == index, jnp.float32(DAMPINGS[index]), damping)
    return quartic, order, damping


def greet_group(n, z, h):
    barrier = pltpu.get_barrier_semaphore()
    pl.semaphore_signal(barrier, inc=1, device_id={"mp": 1 - h}, device_id_type=MESH)
    for o in range(1, n):
        for t in range(2):
            pl.semaphore_signal(
                barrier, inc=1, device_id={"dp": lax.rem(z + o, n), "mp": t}, device_id_type=MESH
            )
    pl.semaphore_wait(barrier, 2 * n - 1)


def remote(src, dst, send, recv, **to):
    return pltpu.make_async_remote_copy(
        src_ref=src, dst_ref=dst, send_sem=send, recv_sem=recv, device_id=to, device_id_type=MESH
    )


def landed(ref, sem):
    pltpu.make_async_copy(ref, ref, sem).wait()


def both_ways(n):
    order = [n // 2]
    for o in range(n // 2 - 1, 0, -1):
        order.extend([o, n - o])
    return order + [0]


QUARTERS = 4
VMEM_BASE = 27 << 20
VMEM_PER_DEVICE = 5 << 10


def step_kernel(
    n, rows, cols,
    table_own, exps, damps, act, grads,
    *refs,
):
    raws = refs[:QUARTERS]
    (
        roots, parts, a_all, b_in, b_all, table_in, table_far, table_smem, acc, shard,
        payload, home_g, slot_g, upd, part_out, t0, q, r, lane_acc, as_r, ar_r,
        as_l, ar_l, b_send, b_recv, f_send, f_recv, t_send, t_recv, loc, h_send, h_recv,
        s_send, s_recv, p_send, p_recv, gs_r, gr_r, gs_l, gr_l, b_load,
    ) = refs[QUARTERS:]
    z = lax.axis_index("dp")
    h = lax.axis_index("mp")
    blocks = rows * cols
    tok = act.shape[0]
    half_tok = tok // 2
    half = BLK // 2
    pieces = BLK // LANE
    loads = []

    def chunk(at):
        return a_all.at[pl.ds(pl.multiple_of(at * tok, tok), tok)]

    for row in range(rows):
        span = pl.ds(pl.multiple_of(row * BLK + h * half, half), half)
        loads.append(pltpu.make_async_copy(
            act.at[:, span], chunk(z).at[:, pl.ds(row * half, half)], loc.at[row]
        ))
    for col in range(cols):
        for jj in range(pieces):
            loads.append(pltpu.make_async_copy(
                grads.at[:, pl.ds(col * BLK + jj * LANE, LANE)],
                b_in.at[jj, :, pl.ds(col * LANE, LANE)],
                b_load.at[jj, col],
            ))
    for one in loads:
        one.start()
    lane = lax.broadcasted_iota(jnp.int32, (8, LANE), 1)
    line = jnp.zeros((8, LANE), jnp.int32)
    for block in range(blocks):
        line = jnp.where(lane == block, table_own[0, block], line)
    table_in[...] = line
    right, left = lax.rem(z + 1, n), lax.rem(z + n - 1, n)
    steps = n // 2
    greet_group(n, z, h)

    ring = []
    for one in loads:
        one.wait()

    def ring_send(step):
        ref_r = chunk(lax.rem(z + n - step, n))
        ref_l = chunk(lax.rem(z + step, n))
        if step == steps - 1:
            ref_r, ref_l = ref_r.at[:, pl.ds(0, half)], ref_l.at[:, pl.ds(half, half)]
        one = remote(ref_r, ref_r, as_r.at[step], ar_r.at[step], dp=right)
        two = remote(ref_l, ref_l, as_l.at[step], ar_l.at[step], dp=left)
        one.start()
        two.start()
        ring.extend([one, two])

    def ring_recv(step):
        dst_r = chunk(lax.rem(z + n - step - 1, n))
        dst_l = chunk(lax.rem(z + step + 1, n))
        if step == steps - 1:
            dst_r, dst_l = dst_r.at[:, pl.ds(0, half)], dst_l.at[:, pl.ds(half, half)]
        landed(dst_r, ar_r.at[step])
        landed(dst_l, ar_l.at[step])

    table = remote(table_in, table_far, t_send, t_recv, mp=1 - h)
    table.start()
    ring_send(0)
    parity = lax.rem(z + h, 2)
    h_rows = pl.ds(pl.multiple_of(h * half_tok, half_tok), half_tok)
    o_rows = pl.ds(pl.multiple_of((1 - h) * half_tok, half_tok), half_tok)

    def piece(i):
        chip = lax.rem(z + parity + 2 * i, n)
        block = b_in.at[chip // 2]
        same = remote(block.at[h_rows], b_all.at[z, h], b_send.at[i, 0], b_recv.at[z], dp=chip, mp=h)
        other = remote(
            block.at[o_rows], b_all.at[z, 1 - h], b_send.at[i, 1], b_recv.at[z], dp=chip, mp=1 - h
        )
        return same, other

    self_chip = parity == 0
    order = []
    for i in range(n // 4):
        order.extend([i, n // 2 - 1 - i])
    for i in order:
        same, other = piece(i)
        if i == 0:
            @pl.when(self_chip)
            def _():
                pltpu.make_async_copy(
                    b_in.at[z // 2].at[h_rows], b_all.at[z, h], b_recv.at[z]
                ).start()

            @pl.when(jnp.logical_not(self_chip))
            def _():
                same.start()
        else:
            same.start()
        other.start()

    def forward(at):
        landed(b_all.at[at, h], b_recv.at[at])
        remote(b_all.at[at, h], b_all.at[at, h], f_send.at[at], f_recv.at[at], mp=1 - h).start()

    def add_source(at, fresh=False):
        landed(b_all.at[at, 1 - h], f_recv.at[at])

        right_side = b_all[at].reshape(tok, cols * LANE)
        for row in range(rows):
            got = dot32(
                chunk(at)[:, row * half:(row + 1) * half], right_side, ((0,), (0,))
            )
            span = pl.ds(row * half, half)
            if fresh:
                acc[span, :] = got
            else:
                acc[span, :] += got

    forward(z)
    for step in range(steps):
        ring_recv(step)
        if step < steps - 1:
            ring_send(step + 1)
        if step == steps - 1:
            forward(lax.rem(z + steps, n))
        else:
            forward(lax.rem(z + step + 1, n))
            forward(lax.rem(z + n - step - 1, n))
        if step == 0:
            add_source(z, True)
        else:
            add_source(lax.rem(z + step, n))
            add_source(lax.rem(z + n - step, n))
    add_source(lax.rem(z + steps, n))
    for row in range(rows):
        for col in range(cols):
            shard[row * cols + col] = acc[
                row * half:(row + 1) * half, col * LANE:(col + 1) * LANE
            ].astype(jnp.bfloat16)

    m = lax.rem(z, 2)
    j = z // 2
    source = z * 2 + h
    spot_of = lambda chip, side: lax.rem(chip + n - SHIFT * side, n)
    my_rows = pl.ds(pl.multiple_of(h * half, half), half)
    my_cols = pl.ds(pl.multiple_of(j * LANE, LANE), LANE)

    def home_move(o):
        chip = lax.rem(z + o, n)
        at = spot_of(chip, m)
        block = (at * blocks + n - 1) // n
        used = jnp.logical_and(block < blocks, (n * block) // blocks == at)
        block = jnp.minimum(block, blocks - 1)
        dst = home_g.at[my_rows, my_cols]
        far = remote(shard.at[block], dst, h_send.at[o], h_recv.at[source], dp=chip, mp=m)
        return used, block, dst, far

    def home_go(o, start):
        used, block, dst, far = home_move(o)
        if o == 0:
            if start:
                @pl.when(jnp.logical_and(used, h == m))
                def _():
                    pltpu.make_async_copy(shard.at[block], dst, h_recv.at[source]).start()

            used = jnp.logical_and(used, h != m)

        @pl.when(used)
        def _():
            if start:
                far.start()
            else:
                far.wait_send()

    for o in both_ways(n):
        home_go(o, True)

    table.wait()
    to_smem = pltpu.make_async_copy(table_far, table_smem, loc.at[1])
    to_smem.start()
    to_smem.wait()

    def slot_move(o):
        chip = lax.rem(z + o, n)
        dst = slot_g.at[my_rows, my_cols]
        return chip, dst, remote(payload.at[chip], dst, s_send.at[o], s_recv.at[source], dp=chip, mp=m)

    for slot in range(n):
        pick = jnp.int32(0)
        filled = jnp.int32(0)
        for block in range(blocks):
            served = jnp.where(m == h, table_own[0, block], table_smem[0, block])
            pick = jnp.where(served == slot, block, pick)
            filled = jnp.where(served == slot, 1, filled)
        part = shard[pick]
        payload[slot] = jnp.where(filled == 1, part, jnp.zeros_like(part))
    for o in both_ways(n):
        chip, dst, far = slot_move(o)
        if o == 0:
            @pl.when(h == m)
            def _():
                pltpu.make_async_copy(payload.at[chip], dst, s_recv.at[source]).start()

            @pl.when(h != m)
            def _():
                far.start()
        else:
            far.start()

    spot = spot_of(z, h)
    own_block = (spot * blocks + n - 1) // n
    busy = jnp.logical_and(own_block < blocks, (n * own_block) // blocks == spot)
    lane_acc[...] = jnp.zeros_like(lane_acc)

    def all_pieces(ref, sems):
        for jj in range(n // 2):
            for t in range(2):
                landed(
                    ref.at[pl.ds(t * half, half), pl.ds(jj * LANE, LANE)],
                    sems.at[(2 * jj + h) * 2 + t],
                )

    def place_of(block, quarter):
        high = BLK // QUARTERS
        return raws[quarter].at[
            pl.ds(pl.multiple_of((block // cols) * high, high), high),
            pl.ds(pl.multiple_of(lax.rem(block, cols) * BLK, BLK), BLK),
        ]

    def quarter_of(quarter):
        high = BLK // QUARTERS
        return upd.at[pl.ds(quarter * high, high)]

    def own_moves(quarter):
        block = jnp.minimum(own_block, blocks - 1)
        src, dst = quarter_of(quarter), place_of(block, quarter)
        return (
            remote(src, dst, gs_r.at[block, quarter], gr_r.at[block, quarter], dp=right),
            remote(src, dst, gs_l.at[block, quarter], gr_l.at[block, quarter], dp=left),
            pltpu.make_async_copy(src, dst, loc.at[2 + quarter]),
        )

    home_slot = table_own[0, jnp.minimum(own_block, blocks - 1)]

    for one in ring:
        one.wait_send()
    gt, m0 = a_all.at[pl.ds(0, BLK)], a_all.at[pl.ds(BLK, BLK)]

    @pl.when(busy)
    def _():
        all_pieces(home_g, h_recv)
        quartic, order_p, damping = picks_of([exps[0, home_slot], damps[0, home_slot]])
        trace = trace_and_turn(home_g, gt, lane_acc)
        root_into(home_g, roots.at[0], order_p, quartic, damping, trace, None, m0, t0, q, r)
        root_into(home_g, roots.at[1], order_p, quartic, damping, trace, gt, m0, t0, q, r)

        def halve(at):
            span = pl.ds(at, STRIPE)
            q[span, :] = dot32(roots[0, span, :], home_g[...]).astype(jnp.bfloat16)

        over_stripes(BLK, halve)
        lane_acc[...] = jnp.zeros_like(lane_acc)

        def finish(at):
            span = pl.ds(at, STRIPE)
            block = dot32(q[span, :], roots[1]).astype(jnp.bfloat16)
            upd[span, :] = block
            wide = block.astype(jnp.float32)
            lane_acc[...] += jnp.sum((wide * wide).reshape(STRIPE // 8, 8, BLK), axis=0)

        over_stripes(BLK, finish)
        for quarter in range(QUARTERS):
            for one in own_moves(quarter):
                one.start()

    tile = lane_acc[:, :LANE]
    for part in range(1, BLK // LANE):
        tile = tile + lane_acc[:, part * LANE:(part + 1) * LANE]
    part_out[...] = tile
    parts[source] = tile

    def hops(side, quarter):
        return n // 2 if (quarter < QUARTERS // 2) == (side == 0) else n // 2 - 1

    def right_block(i):
        x = lax.rem(spot + n - 1, n)
        block = lax.rem(((x + 1) * blocks - 1) // n + blocks - i, blocks)
        return block, lax.rem(spot + n - (n * block) // blocks, n)

    def left_block(i):
        block = lax.rem(((spot + 1) * blocks - 1) // n + 1 + i, blocks)
        return block, lax.rem((n * block) // blocks + n - spot, n)

    def stream(i, quarter, side, phase):
        block, far = (right_block if side == 0 else left_block)(i)
        limit = hops(side, quarter)
        recv = (gr_r if side == 0 else gr_l).at[block, quarter]
        send = (gs_r if side == 0 else gs_l).at[block, quarter]
        ref = place_of(block, quarter)
        go = remote(ref, ref, send, recv, dp=right if side == 0 else left)
        if phase == 0:
            @pl.when(far < limit)
            def _():
                landed(ref, recv)
                go.start()
        elif phase == 1:
            @pl.when(far == limit)
            def _():
                landed(ref, recv)
        else:
            @pl.when(far < limit)
            def _():
                go.wait_send()

    slot_vals = {}

    def slot_first():
        all_pieces(slot_g, s_recv)
        slot_vals["picks"] = picks_of([exps[0, z], damps[0, z]])
        slot_vals["trace"] = trace_and_turn(slot_g, gt, lane_acc)

    def slot_unit(side, body):
        def run():
            quartic, order_p, damping = slot_vals["picks"]
            root_into(
                slot_g, roots.at[side], order_p, quartic, damping, slot_vals["trace"],
                None if side == 0 else gt, m0, t0, q, r, only=body,
            )
        return run

    units = [slot_first] + [slot_unit(side, body) for side in range(2) for body in range(5)]

    def part_move(o, t):
        return remote(
            part_out, parts.at[source], p_send.at[o, t], p_recv.at[source],
            dp=lax.rem(z + o, n), mp=t,
        )

    def part_each(act):
        remote_self = remote(
            part_out, parts.at[source], p_send.at[0, 0], p_recv.at[source], mp=1 - h
        )
        act(remote_self)
        for o in range(1, n):
            for t in range(2):
                act(part_move(o, t))

    most = (blocks + 1) // 2
    for i in range(most):
        for quarter in range(QUARTERS):
            stream(i, quarter, 0, 0)
            stream(i, quarter, 1, 0)
            if i == 0 and quarter == 0:
                part_each(lambda go: go.start())
            if i > 0 and units:
                units.pop(0)()
    for unit in units:
        unit()
    for i in range(most):
        for quarter in range(QUARTERS):
            stream(i, quarter, 0, 1)
            stream(i, quarter, 1, 1)

    for o in range(1, n):
        chip = lax.rem(z + o, n)
        for t in range(2):
            landed(parts.at[chip * 2 + t], p_recv.at[chip * 2 + t])
    landed(parts.at[z * 2 + 1 - h], p_recv.at[z * 2 + 1 - h])
    part_each(lambda go: go.wait_send())
    for i in range(n // 2):
        same, other = piece(i)
        if i == 0:
            @pl.when(jnp.logical_not(self_chip))
            def _():
                same.wait_send()
        else:
            same.wait_send()
        other.wait_send()
    for o in range(n):
        at = lax.rem(z + o, n)
        remote(b_all.at[at, h], b_all.at[at, h], f_send.at[at], f_recv.at[at], mp=1 - h).wait_send()
        home_go(o, False)
        chip, dst, far = slot_move(o)
        if o == 0:
            @pl.when(h != m)
            def _():
                far.wait_send()
        else:
            far.wait_send()

    @pl.when(busy)
    def _():
        for quarter in range(QUARTERS):
            one, two, local = own_moves(quarter)
            one.wait_send()
            two.wait_send()
            local.wait()

    for i in range(most):
        for quarter in range(QUARTERS):
            stream(i, quarter, 0, 2)
            stream(i, quarter, 1, 2)


def run_step(slot_table, exponent_index, damping_index, activations, out_grads, n, rows, cols, devices):
    tok = activations.shape[0]
    dma = pltpu.SemaphoreType.DMA
    smem = pl.BlockSpec(memory_space=pltpu.SMEM)
    vmem = pl.BlockSpec(memory_space=pltpu.VMEM)
    hbm = pl.BlockSpec(memory_space=pltpu.HBM)
    blocks = rows * cols
    half = BLK // 2
    width = rows * half
    pieces = BLK // LANE
    bf = lambda *shape: pltpu.VMEM(shape, jnp.bfloat16)
    steps = n // 2
    return pl.pallas_call(
        functools.partial(step_kernel, n, rows, cols),
        out_shape=(
            *[jax.ShapeDtypeStruct((rows * BLK // QUARTERS, cols * BLK), jnp.bfloat16)] * QUARTERS,
            jax.ShapeDtypeStruct((2, BLK, BLK), jnp.bfloat16),
            jax.ShapeDtypeStruct((2 * n, 8, LANE), jnp.float32),
        ),
        in_specs=[smem, smem, smem, hbm, hbm],
        out_specs=(*[pl.BlockSpec(memory_space=pl.ANY)] * QUARTERS, vmem, vmem),
        scratch_shapes=[
            bf(n * tok, width), bf(pieces, tok, cols * LANE), bf(n, 2, tok // 2, cols * LANE),
            pltpu.VMEM((8, LANE), jnp.int32), pltpu.VMEM((8, LANE), jnp.int32), pltpu.SMEM((8, LANE), jnp.int32),
            pltpu.VMEM((width, cols * LANE), jnp.float32),
            bf(blocks, half, LANE), bf(n, half, LANE), bf(BLK, BLK), bf(BLK, BLK), bf(BLK, BLK),
            pltpu.VMEM((8, LANE), jnp.float32),
            bf(BLK, BLK), bf(BLK, BLK), bf(BLK, BLK),
            pltpu.VMEM((8, BLK), jnp.float32),
            dma((steps,)), dma((steps,)), dma((steps,)), dma((steps,)),
            dma((steps, 2)), dma((n,)), dma((n,)), dma((n,)), dma(()), dma(()),
            dma((2 + QUARTERS,)),
            dma((n,)), dma((2 * n,)), dma((n,)), dma((2 * n,)), dma((n, 2)), dma((2 * n,)),
            dma((blocks, QUARTERS)), dma((blocks, QUARTERS)),
            dma((blocks, QUARTERS)), dma((blocks, QUARTERS)), dma((pieces, cols)),
        ],
        compiler_params=pltpu.CompilerParams(
            collective_id=1, has_side_effects=True, vmem_limit_bytes=VMEM_BASE + VMEM_PER_DEVICE * devices
        ),
        name="shampoo_step",
    )(slot_table, exponent_index, damping_index, activations, out_grads)


def rescale_kernel(entries, parts, *refs):
    out = refs[-1]
    total_sq = jnp.sum(jnp.sum(parts[...], axis=0), keepdims=True)
    scale = lax.rsqrt(total_sq / entries + 1.0)
    g = lax.rem(pl.program_id(0), 2 * QUARTERS)
    for quarter in range(QUARTERS):
        @pl.when(g // 2 == quarter)
        def _(quarter=quarter):
            out[...] = (refs[quarter][...].astype(jnp.float32) * scale).astype(jnp.bfloat16)


def rescaled(raws, parts, entries):
    height, width = raws[0].shape
    high = BLK // QUARTERS // 2
    picks = [
        pl.BlockSpec(
            (high, width),
            lambda g, quarter=quarter: (
                2 * (g // (2 * QUARTERS)) + jnp.clip(g % (2 * QUARTERS) - 2 * quarter, 0, 1), 0
            ),
        )
        for quarter in range(QUARTERS)
    ]
    return pl.pallas_call(
        functools.partial(rescale_kernel, entries),
        out_shape=jax.ShapeDtypeStruct((height * QUARTERS, width), jnp.bfloat16),
        grid=(height * QUARTERS // high,),
        in_specs=[pl.BlockSpec(parts.shape, lambda g: (0, 0, 0))] + picks,
        out_specs=pl.BlockSpec((high, width), lambda g: (g, 0)),
        compiler_params=pltpu.CompilerParams(vmem_limit_bytes=16 << 20),
        cost_estimate=pl.CostEstimate(
            flops=8 * height * width, bytes_accessed=16 * height * width, transcendentals=0
        ),
        name="rescaled",
    )(parts, *raws)


def on_device(devices, activations, out_grads, slot_table, exponent_index, damping_index):
    n = lax.axis_size("dp")
    rows = activations.shape[1] // BLK
    cols = out_grads.shape[1] // BLK
    *raws, roots, parts = run_step(
        slot_table, exponent_index, damping_index, activations, out_grads, n, rows, cols, devices
    )
    entries = rows * BLK * cols * BLK * lax.axis_size("mp")
    update = rescaled(raws, parts, float(entries))
    return (update, roots[None, None])


def solution(mesh):
    placed = (
        P(("member", "dp"), None),
        P(("member", "dp"), "mp"),
        P(("member", "mp"), None),
        P(("member", "mp"), None),
        P(("member", "mp"), None),
    )
    return jax.shard_map(
        functools.partial(on_device, mesh.size),
        mesh=mesh,
        in_specs=placed,
        out_specs=(P("member", "mp"), P(("member", "mp"), "dp", None, None, None)),
        check_vma=False,
    )
```

```python
import functools

import jax
import jax.numpy as jnp
import numpy as np
from jax import lax
from jax.experimental import pallas as pl
from jax.experimental.pallas import tpu as pltpu
from jax.sharding import PartitionSpec as P

BLK = 1024
LANE = 128
ROOT_ORDERS = (2.0, 4.0)
DAMPINGS = (0.03, 0.1, 0.3, 1.0)
SHIFT = 4
MESH = pl.DeviceIdType.MESH


STRIPE = 256


def eye_stripe(at, size):
    row = lax.broadcasted_iota(jnp.int32, (STRIPE, size), 0) + at
    col = lax.broadcasted_iota(jnp.int32, (STRIPE, size), 1)
    return row == col


def dot32(first, second, dims=((1,), (0,))):
    return lax.dot_general(first, second, (dims, ((), ())), preferred_element_type=jnp.float32)


def over_stripes(size, body):
    def step(index, carry):
        body(pl.multiple_of(index * STRIPE, STRIPE))
        return carry

    lax.fori_loop(0, size // STRIPE, step, 0)


def root_into(g, root, order, quartic, damping, trace, gt, m0, t0, q, r, only=None):
    size = g.shape[0]
    shift = damping * (trace / size + 1.0)
    ratio = size / (2.0 * (trace + shift * size))
    base = g if gt is None else gt

    def stat(at):
        rows = pl.ds(at, STRIPE)
        s = dot32(base[rows, :], base[...], ((1,), (1,)))
        on = eye_stripe(at, size)
        scaled = jnp.where(on, s + shift, s) * ratio
        m0[rows, :] = scaled.astype(jnp.bfloat16)
        t0[rows, :] = (jnp.where(on, (order + 1.0) - scaled, -scaled) / order).astype(jnp.bfloat16)

    def square(at):
        rows = pl.ds(at, STRIPE)
        q[rows, :] = dot32(t0[rows, :], t0[...]).astype(jnp.bfloat16)

    def fourth(at):
        rows = pl.ds(at, STRIPE)
        f = dot32(q[rows, :], q[...])
        r[rows, :] = jnp.where(quartic, f, q[rows, :].astype(jnp.float32)).astype(jnp.bfloat16)

    def factor(at):
        rows = pl.ds(at, STRIPE)
        m = dot32(r[rows, :], m0[...])
        on = eye_stripe(at, size)
        q[rows, :] = (jnp.where(on, (order + 1.0) - m, -m) / order).astype(jnp.bfloat16)

    def last(at):
        rows = pl.ds(at, STRIPE)
        root[rows, :] = dot32(t0[rows, :], q[...]).astype(jnp.bfloat16)

    for index, body in enumerate((stat, square, fourth, factor, last)):
        if only is None or only == index:
            over_stripes(size, body)


def trace_and_turn(g, gt, acc):
    size = g.shape[0]
    acc[...] = jnp.zeros_like(acc)

    def body(at):
        rows = pl.ds(at, STRIPE)
        part = g[rows, :]
        wide = part.astype(jnp.float32)
        acc[...] += jnp.sum((wide * wide).reshape(STRIPE // 8, 8, size), axis=0)
        gt[:, rows] = part.T

    over_stripes(size, body)
    return jnp.sum(acc[...])


def picks_of(codes):
    quartic = codes[0] == 1
    order = jnp.where(quartic, ROOT_ORDERS[1], ROOT_ORDERS[0])
    damping = jnp.float32(DAMPINGS[0])
    for index in range(1, len(DAMPINGS)):
        damping = jnp.where(codes[1] == index, jnp.float32(DAMPINGS[index]), damping)
    return quartic, order, damping


def greet_group(n, z, h):
    barrier = pltpu.get_barrier_semaphore()
    pl.semaphore_signal(barrier, inc=1, device_id={"mp": 1 - h}, device_id_type=MESH)
    for o in range(1, n):
        for t in range(2):
            pl.semaphore_signal(
                barrier, inc=1, device_id={"dp": lax.rem(z + o, n), "mp": t}, device_id_type=MESH
            )
    pl.semaphore_wait(barrier, 2 * n - 1)


def remote(src, dst, send, recv, **to):
    return pltpu.make_async_remote_copy(
        src_ref=src, dst_ref=dst, send_sem=send, recv_sem=recv, device_id=to, device_id_type=MESH
    )


def landed(ref, sem):
    pltpu.make_async_copy(ref, ref, sem).wait()


def both_ways(n):
    order = [n // 2]
    for o in range(n // 2 - 1, 0, -1):
        order.extend([o, n - o])
    return order + [0]


QUARTERS = 4
SLOT_MASK = 255
VMEM_BASE = 27 << 20
VMEM_PER_DEVICE = 5 << 10
RESCALE_LIMIT = 28 << 20


def step_kernel(
    n, rows, cols,
    packed, act, grads,
    *refs,
):
    raws = refs[:QUARTERS]
    (
        roots, parts, a_all, b_in, b_all, table_in, table_far, table_smem, acc, shard,
        payload, home_g, slot_g, upd, part_out, t0, q, r, lane_acc, as_r, ar_r,
        as_l, ar_l, b_send, b_recv, f_send, f_recv, t_send, t_recv, loc, h_send, h_recv,
        s_send, s_recv, p_send, p_recv, gs_r, gr_r, gs_l, gr_l, b_load,
    ) = refs[QUARTERS:]
    z = lax.axis_index("dp")
    h = lax.axis_index("mp")
    blocks = rows * cols
    tok = act.shape[0]
    half_tok = tok // 2
    half = BLK // 2
    pieces = BLK // LANE
    loads = []

    def chunk(at):
        return a_all.at[pl.ds(pl.multiple_of(at * tok, tok), tok)]

    for row in range(rows):
        span = pl.ds(pl.multiple_of(row * BLK + h * half, half), half)
        loads.append(pltpu.make_async_copy(
            act.at[:, span], chunk(z).at[:, pl.ds(row * half, half)], loc.at[row]
        ))
    for col in range(cols):
        for jj in range(pieces):
            loads.append(pltpu.make_async_copy(
                grads.at[:, pl.ds(col * BLK + jj * LANE, LANE)],
                b_in.at[jj, :, pl.ds(col * LANE, LANE)],
                b_load.at[jj, col],
            ))
    for one in loads:
        one.start()
    def codes_at(slot):
        word = packed[0, slot]
        return (word >> 8) & 15, (word >> 12) & 15

    lane = lax.broadcasted_iota(jnp.int32, (8, LANE), 1)
    line = jnp.zeros((8, LANE), jnp.int32)
    for block in range(blocks):
        line = jnp.where(lane == block, packed[0, block] & SLOT_MASK, line)
    table_in[...] = line
    right, left = lax.rem(z + 1, n), lax.rem(z + n - 1, n)
    steps = n // 2
    greet_group(n, z, h)

    ring = []
    for one in loads:
        one.wait()

    def ring_part(at, row):
        return chunk(at).at[:, pl.ds(row * half, half)]

    def ring_rows(step, side):
        return (side,) if step == steps - 1 else tuple(range(rows))

    def ring_send(step, side, row):
        at = lax.rem(z + n - step, n) if side == 0 else lax.rem(z + step, n)
        ref = ring_part(at, row)
        send, recv, to = (as_r, ar_r, right) if side == 0 else (as_l, ar_l, left)
        one = remote(ref, ref, send.at[step, row], recv.at[step, row], dp=to)
        one.start()
        ring.append(one)

    def ring_recv(step, side, row):
        at = lax.rem(z + n - step - 1, n) if side == 0 else lax.rem(z + step + 1, n)
        landed(ring_part(at, row), (ar_r if side == 0 else ar_l).at[step, row])

    table = remote(table_in, table_far, t_send, t_recv, mp=1 - h)
    table.start()
    for row in range(rows):
        for side in range(2):
            ring_send(0, side, row)
    parity = lax.rem(z + h, 2)
    h_rows = pl.ds(pl.multiple_of(h * half_tok, half_tok), half_tok)
    o_rows = pl.ds(pl.multiple_of((1 - h) * half_tok, half_tok), half_tok)

    def piece(i):
        chip = lax.rem(z + parity + 2 * i, n)
        block = b_in.at[chip // 2]
        same = remote(block.at[h_rows], b_all.at[z, h], b_send.at[i, 0], b_recv.at[z], dp=chip, mp=h)
        other = remote(
            block.at[o_rows], b_all.at[z, 1 - h], b_send.at[i, 1], b_recv.at[z], dp=chip, mp=1 - h
        )
        return same, other

    self_chip = parity == 0
    order = []
    for i in range(n // 4):
        order.extend([i, n // 2 - 1 - i])
    for i in order:
        same, other = piece(i)
        if i == 0:
            @pl.when(self_chip)
            def _():
                pltpu.make_async_copy(
                    b_in.at[z // 2].at[h_rows], b_all.at[z, h], b_recv.at[z]
                ).start()

            @pl.when(jnp.logical_not(self_chip))
            def _():
                same.start()
        else:
            same.start()
        other.start()

    def forward(at):
        landed(b_all.at[at, h], b_recv.at[at])
        remote(b_all.at[at, h], b_all.at[at, h], f_send.at[at], f_recv.at[at], mp=1 - h).start()

    def add_source(at, fresh=False):
        landed(b_all.at[at, 1 - h], f_recv.at[at])

        right_side = b_all[at].reshape(tok, cols * LANE)
        for row in range(rows):
            got = dot32(
                chunk(at)[:, row * half:(row + 1) * half], right_side, ((0,), (0,))
            )
            span = pl.ds(row * half, half)
            if fresh:
                acc[span, :] = got
            else:
                acc[span, :] += got

    forward(z)
    for step in range(steps):
        if step == steps - 1:
            add_source(lax.rem(z + step, n))
            add_source(lax.rem(z + n - step, n))
        for row in range(rows):
            for side in range(2):
                if row in ring_rows(step, side):
                    ring_recv(step, side, row)
                if step < steps - 1 and row in ring_rows(step + 1, side):
                    ring_send(step + 1, side, row)
        if step == steps - 1:
            forward(lax.rem(z + steps, n))
        else:
            forward(lax.rem(z + step + 1, n))
            forward(lax.rem(z + n - step - 1, n))
        if step == 0:
            add_source(z, True)
        elif step < steps - 1:
            add_source(lax.rem(z + step, n))
            add_source(lax.rem(z + n - step, n))
    add_source(lax.rem(z + steps, n))
    for row in range(rows):
        for col in range(cols):
            shard[row * cols + col] = acc[
                row * half:(row + 1) * half, col * LANE:(col + 1) * LANE
            ].astype(jnp.bfloat16)

    m = lax.rem(z, 2)
    j = z // 2
    source = z * 2 + h
    spot_of = lambda chip, side: lax.rem(chip + n - SHIFT * side, n)
    my_rows = pl.ds(pl.multiple_of(h * half, half), half)
    my_cols = pl.ds(pl.multiple_of(j * LANE, LANE), LANE)

    def home_move(o):
        chip = lax.rem(z + o, n)
        at = spot_of(chip, m)
        block = (at * blocks + n - 1) // n
        used = jnp.logical_and(block < blocks, (n * block) // blocks == at)
        block = jnp.minimum(block, blocks - 1)
        dst = home_g.at[my_rows, my_cols]
        far = remote(shard.at[block], dst, h_send.at[o], h_recv.at[source], dp=chip, mp=m)
        return used, block, dst, far

    def home_go(o, start):
        used, block, dst, far = home_move(o)
        if o == 0:
            if start:
                @pl.when(jnp.logical_and(used, h == m))
                def _():
                    pltpu.make_async_copy(shard.at[block], dst, h_recv.at[source]).start()

            used = jnp.logical_and(used, h != m)

        @pl.when(used)
        def _():
            if start:
                far.start()
            else:
                far.wait_send()

    for o in both_ways(n):
        home_go(o, True)

    table.wait()
    to_smem = pltpu.make_async_copy(table_far, table_smem, loc.at[1])
    to_smem.start()
    to_smem.wait()

    def slot_move(o):
        chip = lax.rem(z + o, n)
        dst = slot_g.at[my_rows, my_cols]
        return chip, dst, remote(payload.at[chip], dst, s_send.at[o], s_recv.at[source], dp=chip, mp=m)

    for slot in range(n):
        pick = jnp.int32(0)
        filled = jnp.int32(0)
        for block in range(blocks):
            served = jnp.where(m == h, packed[0, block] & SLOT_MASK, table_smem[0, block])
            pick = jnp.where(served == slot, block, pick)
            filled = jnp.where(served == slot, 1, filled)
        part = shard[pick]
        payload[slot] = jnp.where(filled == 1, part, jnp.zeros_like(part))
    for o in both_ways(n):
        chip, dst, far = slot_move(o)
        if o == 0:
            @pl.when(h == m)
            def _():
                pltpu.make_async_copy(payload.at[chip], dst, s_recv.at[source]).start()

            @pl.when(h != m)
            def _():
                far.start()
        else:
            far.start()

    spot = spot_of(z, h)
    own_block = (spot * blocks + n - 1) // n
    busy = jnp.logical_and(own_block < blocks, (n * own_block) // blocks == spot)
    lane_acc[...] = jnp.zeros_like(lane_acc)

    def all_pieces(ref, sems):
        for jj in range(n // 2):
            for t in range(2):
                landed(
                    ref.at[pl.ds(t * half, half), pl.ds(jj * LANE, LANE)],
                    sems.at[(2 * jj + h) * 2 + t],
                )

    def place_of(block, quarter):
        high = BLK // QUARTERS
        return raws[quarter].at[
            pl.ds(pl.multiple_of((block // cols) * high, high), high),
            pl.ds(pl.multiple_of(lax.rem(block, cols) * BLK, BLK), BLK),
        ]

    def quarter_of(quarter):
        high = BLK // QUARTERS
        return upd.at[pl.ds(quarter * high, high)]

    def own_moves(quarter):
        block = jnp.minimum(own_block, blocks - 1)
        src, dst = quarter_of(quarter), place_of(block, quarter)
        return (
            remote(src, dst, gs_r.at[block, quarter], gr_r.at[block, quarter], dp=right),
            remote(src, dst, gs_l.at[block, quarter], gr_l.at[block, quarter], dp=left),
            pltpu.make_async_copy(src, dst, loc.at[2 + quarter]),
        )

    home_slot = packed[0, jnp.minimum(own_block, blocks - 1)] & SLOT_MASK

    for one in ring:
        one.wait_send()
    gt, m0 = a_all.at[pl.ds(0, BLK)], a_all.at[pl.ds(BLK, BLK)]

    @pl.when(busy)
    def _():
        all_pieces(home_g, h_recv)
        quartic, order_p, damping = picks_of(codes_at(home_slot))
        trace = trace_and_turn(home_g, gt, lane_acc)
        root_into(home_g, roots.at[0], order_p, quartic, damping, trace, None, m0, t0, q, r)
        root_into(home_g, roots.at[1], order_p, quartic, damping, trace, gt, m0, t0, q, r)

        def halve(at):
            span = pl.ds(at, STRIPE)
            q[span, :] = dot32(roots[0, span, :], home_g[...]).astype(jnp.bfloat16)

        over_stripes(BLK, halve)
        lane_acc[...] = jnp.zeros_like(lane_acc)

        def finish(at):
            span = pl.ds(at, STRIPE)
            block = dot32(q[span, :], roots[1]).astype(jnp.bfloat16)
            upd[span, :] = block
            wide = block.astype(jnp.float32)
            lane_acc[...] += jnp.sum((wide * wide).reshape(STRIPE // 8, 8, BLK), axis=0)

        over_stripes(BLK, finish)
        for quarter in range(QUARTERS):
            for one in own_moves(quarter):
                one.start()

    tile = lane_acc[:, :LANE]
    for part in range(1, BLK // LANE):
        tile = tile + lane_acc[:, part * LANE:(part + 1) * LANE]
    part_out[...] = tile
    parts[source] = tile

    def hops(side, quarter):
        return n // 2 if (quarter < QUARTERS // 2) == (side == 0) else n // 2 - 1

    def right_block(i):
        x = lax.rem(spot + n - 1, n)
        block = lax.rem(((x + 1) * blocks - 1) // n + blocks - i, blocks)
        return block, lax.rem(spot + n - (n * block) // blocks, n)

    def left_block(i):
        block = lax.rem(((spot + 1) * blocks - 1) // n + 1 + i, blocks)
        return block, lax.rem((n * block) // blocks + n - spot, n)

    def stream(i, quarter, side, phase):
        block, far = (right_block if side == 0 else left_block)(i)
        limit = hops(side, quarter)
        recv = (gr_r if side == 0 else gr_l).at[block, quarter]
        send = (gs_r if side == 0 else gs_l).at[block, quarter]
        ref = place_of(block, quarter)
        go = remote(ref, ref, send, recv, dp=right if side == 0 else left)
        if phase == 0:
            @pl.when(far < limit)
            def _():
                landed(ref, recv)
                go.start()
        elif phase == 1:
            @pl.when(far == limit)
            def _():
                landed(ref, recv)
        else:
            @pl.when(far < limit)
            def _():
                go.wait_send()

    slot_vals = {}

    def slot_first():
        all_pieces(slot_g, s_recv)
        slot_vals["picks"] = picks_of(codes_at(z))
        slot_vals["trace"] = trace_and_turn(slot_g, gt, lane_acc)

    def slot_unit(side, body):
        def run():
            quartic, order_p, damping = slot_vals["picks"]
            root_into(
                slot_g, roots.at[side], order_p, quartic, damping, slot_vals["trace"],
                None if side == 0 else gt, m0, t0, q, r, only=body,
            )
        return run

    units = [slot_first] + [slot_unit(side, body) for side in range(2) for body in range(5)]

    def part_move(o, t):
        return remote(
            part_out, parts.at[source], p_send.at[o, t], p_recv.at[source],
            dp=lax.rem(z + o, n), mp=t,
        )

    def part_each(act):
        remote_self = remote(
            part_out, parts.at[source], p_send.at[0, 0], p_recv.at[source], mp=1 - h
        )
        act(remote_self)
        for o in range(1, n):
            for t in range(2):
                act(part_move(o, t))

    most = (blocks + 1) // 2
    for i in range(most):
        for quarter in range(QUARTERS):
            stream(i, quarter, 0, 0)
            stream(i, quarter, 1, 0)
            if i == 0 and quarter == 0:
                part_each(lambda go: go.start())
            if i > 0 and units:
                units.pop(0)()
    for unit in units:
        unit()
    for i in range(most):
        for quarter in range(QUARTERS):
            stream(i, quarter, 0, 1)
            stream(i, quarter, 1, 1)

    for o in range(1, n):
        chip = lax.rem(z + o, n)
        for t in range(2):
            landed(parts.at[chip * 2 + t], p_recv.at[chip * 2 + t])
    landed(parts.at[z * 2 + 1 - h], p_recv.at[z * 2 + 1 - h])
    part_each(lambda go: go.wait_send())
    for i in range(n // 2):
        same, other = piece(i)
        if i == 0:
            @pl.when(jnp.logical_not(self_chip))
            def _():
                same.wait_send()
        else:
            same.wait_send()
        other.wait_send()
    for o in range(n):
        at = lax.rem(z + o, n)
        remote(b_all.at[at, h], b_all.at[at, h], f_send.at[at], f_recv.at[at], mp=1 - h).wait_send()
        home_go(o, False)
        chip, dst, far = slot_move(o)
        if o == 0:
            @pl.when(h != m)
            def _():
                far.wait_send()
        else:
            far.wait_send()

    @pl.when(busy)
    def _():
        for quarter in range(QUARTERS):
            one, two, local = own_moves(quarter)
            one.wait_send()
            two.wait_send()
            local.wait()

    for i in range(most):
        for quarter in range(QUARTERS):
            stream(i, quarter, 0, 2)
            stream(i, quarter, 1, 2)


def run_step(packed, activations, out_grads, n, rows, cols, devices):
    tok = activations.shape[0]
    dma = pltpu.SemaphoreType.DMA
    smem = pl.BlockSpec(memory_space=pltpu.SMEM)
    vmem = pl.BlockSpec(memory_space=pltpu.VMEM)
    hbm = pl.BlockSpec(memory_space=pltpu.HBM)
    blocks = rows * cols
    half = BLK // 2
    width = rows * half
    pieces = BLK // LANE
    bf = lambda *shape: pltpu.VMEM(shape, jnp.bfloat16)
    steps = n // 2
    return pl.pallas_call(
        functools.partial(step_kernel, n, rows, cols),
        out_shape=(
            *[jax.ShapeDtypeStruct((rows * BLK // QUARTERS, cols * BLK), jnp.bfloat16)] * QUARTERS,
            jax.ShapeDtypeStruct((2, BLK, BLK), jnp.bfloat16),
            jax.ShapeDtypeStruct((2 * n, 8, LANE), jnp.float32),
        ),
        in_specs=[smem, hbm, hbm],
        out_specs=(*[pl.BlockSpec(memory_space=pl.ANY)] * QUARTERS, vmem, vmem),
        scratch_shapes=[
            bf(n * tok, width), bf(pieces, tok, cols * LANE), bf(n, 2, tok // 2, cols * LANE),
            pltpu.VMEM((8, LANE), jnp.int32), pltpu.VMEM((8, LANE), jnp.int32), pltpu.SMEM((8, LANE), jnp.int32),
            pltpu.VMEM((width, cols * LANE), jnp.float32),
            bf(blocks, half, LANE), bf(n, half, LANE), bf(BLK, BLK), bf(BLK, BLK), bf(BLK, BLK),
            pltpu.VMEM((8, LANE), jnp.float32),
            bf(BLK, BLK), bf(BLK, BLK), bf(BLK, BLK),
            pltpu.VMEM((8, BLK), jnp.float32),
            dma((steps, rows)), dma((steps, rows)), dma((steps, rows)), dma((steps, rows)),
            dma((steps, 2)), dma((n,)), dma((n,)), dma((n,)), dma(()), dma(()),
            dma((2 + QUARTERS,)),
            dma((n,)), dma((2 * n,)), dma((n,)), dma((2 * n,)), dma((n, 2)), dma((2 * n,)),
            dma((blocks, QUARTERS)), dma((blocks, QUARTERS)),
            dma((blocks, QUARTERS)), dma((blocks, QUARTERS)), dma((pieces, cols)),
        ],
        compiler_params=pltpu.CompilerParams(
            collective_id=1, has_side_effects=True, vmem_limit_bytes=VMEM_BASE + VMEM_PER_DEVICE * devices
        ),
        name="shampoo_step",
    )(packed, activations, out_grads)


def rescale_kernel(entries, high, parts, *refs):
    raws, (out, buffers, sems) = refs[:QUARTERS], refs[QUARTERS:]
    total_sq = jnp.sum(jnp.sum(parts[...], axis=0), keepdims=True)
    scale = lax.rsqrt(total_sq / entries + 1.0)
    groups = raws[0].shape[0] // high
    per_row = BLK // QUARTERS // high

    def out_copy(quarter, group):
        at = (group // per_row) * BLK + quarter * (BLK // QUARTERS) + lax.rem(group, per_row) * high
        return pltpu.make_async_copy(
            buffers.at[group], out.at[pl.ds(pl.multiple_of(at, high), high)], sems.at[group]
        )

    for quarter in range(QUARTERS):
        def step(group, carry, quarter=quarter):
            if quarter > 0:
                out_copy(quarter - 1, group).wait()
            span = pl.ds(pl.multiple_of(group * high, high), high)
            wide = raws[quarter][span, :].astype(jnp.float32)
            buffers[group] = (wide * scale).astype(jnp.bfloat16)
            out_copy(quarter, group).start()
            return carry

        lax.fori_loop(0, groups, step, 0)
    for group in range(groups):
        out_copy(QUARTERS - 1, group).wait()


def rescaled(raws, parts, entries):
    height, width = raws[0].shape
    high = BLK // QUARTERS // 2
    vmem = pl.BlockSpec(memory_space=pltpu.VMEM)
    return pl.pallas_call(
        functools.partial(rescale_kernel, entries, high),
        out_shape=jax.ShapeDtypeStruct((height * QUARTERS, width), jnp.bfloat16),
        in_specs=[vmem] * (1 + QUARTERS),
        out_specs=pl.BlockSpec(memory_space=pl.ANY),
        scratch_shapes=[
            pltpu.VMEM((height // high, high, width), jnp.bfloat16),
            pltpu.SemaphoreType.DMA((height // high,)),
        ],
        compiler_params=pltpu.CompilerParams(vmem_limit_bytes=RESCALE_LIMIT),
        cost_estimate=pl.CostEstimate(
            flops=8 * height * width, bytes_accessed=16 * height * width, transcendentals=0
        ),
        name="rescaled",
    )(parts, *raws)


def on_device(devices, activations, out_grads, slot_table, exponent_index, damping_index):
    n = lax.axis_size("dp")
    rows = activations.shape[1] // BLK
    cols = out_grads.shape[1] // BLK
    *raws, roots, parts = run_step(
        slot_table + exponent_index * 256 + damping_index * 4096, activations, out_grads, n, rows, cols, devices
    )
    entries = rows * BLK * cols * BLK * lax.axis_size("mp")
    update = rescaled(raws, parts, float(entries))
    return (update, roots[None, None])


def solution(mesh):
    placed = (
        P(("member", "dp"), None),
        P(("member", "dp"), "mp"),
        P(("member", "mp"), None),
        P(("member", "mp"), None),
        P(("member", "mp"), None),
    )
    return jax.shard_map(
        functools.partial(on_device, mesh.size),
        mesh=mesh,
        in_specs=placed,
        out_specs=(P("member", "mp"), P(("member", "mp"), "dp", None, None, None)),
        check_vma=False,
    )
```

```python
import functools

import jax
import jax.numpy as jnp
import numpy as np
from jax import lax
from jax.experimental import pallas as pl
from jax.experimental.pallas import tpu as pltpu
from jax.sharding import PartitionSpec as P

BLK = 1024
LANE = 128
ROOT_ORDERS = (2.0, 4.0)
DAMPINGS = (0.03, 0.1, 0.3, 1.0)
SHIFT = 4
MESH = pl.DeviceIdType.MESH


STRIPE = 256


def eye_stripe(at, size):
    row = lax.broadcasted_iota(jnp.int32, (STRIPE, size), 0) + at
    col = lax.broadcasted_iota(jnp.int32, (STRIPE, size), 1)
    return row == col


def dot32(first, second, dims=((1,), (0,))):
    return lax.dot_general(first, second, (dims, ((), ())), preferred_element_type=jnp.float32)


def over_stripes(size, body):
    def step(index, carry):
        body(pl.multiple_of(index * STRIPE, STRIPE))
        return carry

    lax.fori_loop(0, size // STRIPE, step, 0)


def root_into(g, root, order, quartic, damping, trace, gt, m0, t0, q, r, only=None):
    size = g.shape[0]
    shift = damping * (trace / size + 1.0)
    ratio = size / (2.0 * (trace + shift * size))
    base = g if gt is None else gt

    def stat(at):
        rows = pl.ds(at, STRIPE)
        s = dot32(base[rows, :], base[...], ((1,), (1,)))
        on = eye_stripe(at, size)
        scaled = jnp.where(on, s + shift, s) * ratio
        m0[rows, :] = scaled.astype(jnp.bfloat16)
        t0[rows, :] = (jnp.where(on, (order + 1.0) - scaled, -scaled) / order).astype(jnp.bfloat16)

    def square(at):
        rows = pl.ds(at, STRIPE)
        q[rows, :] = dot32(t0[rows, :], t0[...]).astype(jnp.bfloat16)

    def fourth(at):
        rows = pl.ds(at, STRIPE)
        f = dot32(q[rows, :], q[...])
        r[rows, :] = jnp.where(quartic, f, q[rows, :].astype(jnp.float32)).astype(jnp.bfloat16)

    def factor(at):
        rows = pl.ds(at, STRIPE)
        m = dot32(r[rows, :], m0[...])
        on = eye_stripe(at, size)
        q[rows, :] = (jnp.where(on, (order + 1.0) - m, -m) / order).astype(jnp.bfloat16)

    def last(at):
        rows = pl.ds(at, STRIPE)
        root[rows, :] = dot32(t0[rows, :], q[...]).astype(jnp.bfloat16)

    for index, body in enumerate((stat, square, fourth, factor, last)):
        if only is None or only == index:
            over_stripes(size, body)


def trace_and_turn(g, gt, acc):
    size = g.shape[0]
    acc[...] = jnp.zeros_like(acc)

    def body(at):
        rows = pl.ds(at, STRIPE)
        part = g[rows, :]
        wide = part.astype(jnp.float32)
        acc[...] += jnp.sum((wide * wide).reshape(STRIPE // 8, 8, size), axis=0)
        gt[:, rows] = part.T

    over_stripes(size, body)
    return jnp.sum(acc[...])


def picks_of(codes):
    quartic = codes[0] == 1
    order = jnp.where(quartic, ROOT_ORDERS[1], ROOT_ORDERS[0])
    damping = jnp.float32(DAMPINGS[0])
    for index in range(1, len(DAMPINGS)):
        damping = jnp.where(codes[1] == index, jnp.float32(DAMPINGS[index]), damping)
    return quartic, order, damping


def greet_neighbours(n, z, h):
    barrier = pltpu.get_barrier_semaphore()
    pl.semaphore_signal(barrier, inc=1, device_id={"mp": 1 - h}, device_id_type=MESH)
    for o in (1, n - 1):
        pl.semaphore_signal(
            barrier, inc=1, device_id={"dp": lax.rem(z + o, n)}, device_id_type=MESH
        )
    pl.semaphore_wait(barrier, 3)


def remote(src, dst, send, recv, **to):
    return pltpu.make_async_remote_copy(
        src_ref=src, dst_ref=dst, send_sem=send, recv_sem=recv, device_id=to, device_id_type=MESH
    )


def landed(ref, sem):
    pltpu.make_async_copy(ref, ref, sem).wait()


def both_ways(n):
    order = [n // 2]
    for o in range(n // 2 - 1, 0, -1):
        order.extend([o, n - o])
    return order + [0]


QUARTERS = 4
SLOT_MASK = 255
VMEM_BASE = 27 << 20
VMEM_PER_DEVICE = 5 << 10
RESCALE_BASE = 22 << 20


def step_kernel(
    n, rows, cols,
    packed, act, grads,
    *refs,
):
    raws = refs[:QUARTERS]
    (
        roots, parts, a_all, b_in, b_all, table_in, table_far, table_smem, acc, shard,
        payload, home_g, slot_g, upd, part_out, t0, q, r, lane_acc, as_r, ar_r,
        as_l, ar_l, b_send, b_recv, f_send, f_recv, t_send, t_recv, loc, h_send, h_recv,
        s_send, s_recv, p_send, p_recv, gs_r, gr_r, gs_l, gr_l, b_load, tok_r, tok_l,
    ) = refs[QUARTERS:]
    z = lax.axis_index("dp")
    h = lax.axis_index("mp")
    blocks = rows * cols
    tok = act.shape[0]
    half_tok = tok // 2
    half = BLK // 2
    pieces = BLK // LANE
    loads = []

    def chunk(at):
        return a_all.at[pl.ds(pl.multiple_of(at * tok, tok), tok)]

    for row in range(rows):
        span = pl.ds(pl.multiple_of(row * BLK + h * half, half), half)
        loads.append(pltpu.make_async_copy(
            act.at[:, span], chunk(z).at[:, pl.ds(row * half, half)], loc.at[row]
        ))
    for col in range(cols):
        for jj in range(pieces):
            loads.append(pltpu.make_async_copy(
                grads.at[:, pl.ds(col * BLK + jj * LANE, LANE)],
                b_in.at[jj, :, pl.ds(col * LANE, LANE)],
                b_load.at[jj, col],
            ))
    for one in loads:
        one.start()
    def codes_at(slot):
        word = packed[0, slot]
        return (word >> 8) & 15, (word >> 12) & 15

    lane = lax.broadcasted_iota(jnp.int32, (8, LANE), 1)
    line = jnp.zeros((8, LANE), jnp.int32)
    for block in range(blocks):
        line = jnp.where(lane == block, packed[0, block] & SLOT_MASK, line)
    table_in[...] = line
    right, left = lax.rem(z + 1, n), lax.rem(z + n - 1, n)
    steps = n // 2
    greet_neighbours(n, z, h)

    def tell(t):
        pl.semaphore_signal(tok_r.at[t], inc=1, device_id={"dp": right}, device_id_type=MESH)
        if t < steps - 1:
            pl.semaphore_signal(tok_l.at[t], inc=1, device_id={"dp": left}, device_id_type=MESH)

    def hear(t):
        pl.semaphore_wait(tok_r.at[t], 1)
        if t < steps - 1:
            pl.semaphore_wait(tok_l.at[t], 1)

    tell(0)

    ring = []
    for one in loads:
        one.wait()

    def ring_part(at, row):
        return chunk(at).at[:, pl.ds(row * half, half)]

    def ring_rows(step, side):
        return (side,) if step == steps - 1 else tuple(range(rows))

    def ring_send(step, side, row):
        at = lax.rem(z + n - step, n) if side == 0 else lax.rem(z + step, n)
        ref = ring_part(at, row)
        send, recv, to = (as_r, ar_r, right) if side == 0 else (as_l, ar_l, left)
        one = remote(ref, ref, send.at[step, row], recv.at[step, row], dp=to)
        one.start()
        ring.append(one)

    def ring_recv(step, side, row):
        at = lax.rem(z + n - step - 1, n) if side == 0 else lax.rem(z + step + 1, n)
        landed(ring_part(at, row), (ar_r if side == 0 else ar_l).at[step, row])

    table = remote(table_in, table_far, t_send, t_recv, mp=1 - h)
    table.start()
    for row in range(rows):
        for side in range(2):
            ring_send(0, side, row)
    parity = lax.rem(z + h, 2)
    h_rows = pl.ds(pl.multiple_of(h * half_tok, half_tok), half_tok)
    o_rows = pl.ds(pl.multiple_of((1 - h) * half_tok, half_tok), half_tok)

    def piece(o):
        chip = lax.rem(z + o, n)
        block = b_in.at[chip // 2]
        same = remote(block.at[h_rows], b_all.at[z, h], b_send.at[o, 0], b_recv.at[z], dp=chip, mp=h)
        other = remote(
            block.at[o_rows], b_all.at[z, 1 - h], b_send.at[o, 1], b_recv.at[z], dp=chip, mp=1 - h
        )
        return same, other

    def piece_go(o, start):
        @pl.when(parity == o % 2)
        def _():
            same, other = piece(o)
            if o == 0:
                if start:
                    pltpu.make_async_copy(
                        b_in.at[z // 2].at[h_rows], b_all.at[z, h], b_recv.at[z]
                    ).start()
            elif start:
                same.start()
            else:
                same.wait_send()
            if start:
                other.start()
            else:
                other.wait_send()

    piece_go(0, True)
    for t in range(steps):
        hear(t)
        if t < steps - 1:
            tell(t + 1)
            piece_go(t + 1, True)
            piece_go(n - t - 1, True)
        else:
            piece_go(steps, True)

    def forward(at):
        landed(b_all.at[at, h], b_recv.at[at])
        remote(b_all.at[at, h], b_all.at[at, h], f_send.at[at], f_recv.at[at], mp=1 - h).start()

    def add_source(at, fresh=False):
        landed(b_all.at[at, 1 - h], f_recv.at[at])

        right_side = b_all[at].reshape(tok, cols * LANE)
        for row in range(rows):
            got = dot32(
                chunk(at)[:, row * half:(row + 1) * half], right_side, ((0,), (0,))
            )
            span = pl.ds(row * half, half)
            if fresh:
                acc[span, :] = got
            else:
                acc[span, :] += got

    forward(z)
    for step in range(steps):
        if step == steps - 1:
            add_source(lax.rem(z + step, n))
            add_source(lax.rem(z + n - step, n))
        for row in range(rows):
            for side in range(2):
                if row in ring_rows(step, side):
                    ring_recv(step, side, row)
                if step < steps - 1 and row in ring_rows(step + 1, side):
                    ring_send(step + 1, side, row)
        if step == steps - 1:
            forward(lax.rem(z + steps, n))
        else:
            forward(lax.rem(z + step + 1, n))
            forward(lax.rem(z + n - step - 1, n))
        if step == 0:
            add_source(z, True)
        elif step < steps - 1:
            add_source(lax.rem(z + step, n))
            add_source(lax.rem(z + n - step, n))
    add_source(lax.rem(z + steps, n))
    for row in range(rows):
        for col in range(cols):
            shard[row * cols + col] = acc[
                row * half:(row + 1) * half, col * LANE:(col + 1) * LANE
            ].astype(jnp.bfloat16)

    m = lax.rem(z, 2)
    j = z // 2
    source = z * 2 + h
    spot_of = lambda chip, side: lax.rem(chip + n - SHIFT * side, n)
    my_rows = pl.ds(pl.multiple_of(h * half, half), half)
    my_cols = pl.ds(pl.multiple_of(j * LANE, LANE), LANE)

    def home_move(o):
        chip = lax.rem(z + o, n)
        at = spot_of(chip, m)
        block = (at * blocks + n - 1) // n
        used = jnp.logical_and(block < blocks, (n * block) // blocks == at)
        block = jnp.minimum(block, blocks - 1)
        dst = home_g.at[my_rows, my_cols]
        far = remote(shard.at[block], dst, h_send.at[o], h_recv.at[source], dp=chip, mp=m)
        return used, block, dst, far

    def home_go(o, start):
        used, block, dst, far = home_move(o)
        if o == 0:
            if start:
                @pl.when(jnp.logical_and(used, h == m))
                def _():
                    pltpu.make_async_copy(shard.at[block], dst, h_recv.at[source]).start()

            used = jnp.logical_and(used, h != m)

        @pl.when(used)
        def _():
            if start:
                far.start()
            else:
                far.wait_send()

    for o in both_ways(n):
        home_go(o, True)

    table.wait()
    to_smem = pltpu.make_async_copy(table_far, table_smem, loc.at[1])
    to_smem.start()
    to_smem.wait()

    def slot_move(o):
        chip = lax.rem(z + o, n)
        dst = slot_g.at[my_rows, my_cols]
        return chip, dst, remote(payload.at[chip], dst, s_send.at[o], s_recv.at[source], dp=chip, mp=m)

    for slot in range(n):
        pick = jnp.int32(0)
        filled = jnp.int32(0)
        for block in range(blocks):
            served = jnp.where(m == h, packed[0, block] & SLOT_MASK, table_smem[0, block])
            pick = jnp.where(served == slot, block, pick)
            filled = jnp.where(served == slot, 1, filled)
        part = shard[pick]
        payload[slot] = jnp.where(filled == 1, part, jnp.zeros_like(part))
    for o in both_ways(n):
        chip, dst, far = slot_move(o)
        if o == 0:
            @pl.when(h == m)
            def _():
                pltpu.make_async_copy(payload.at[chip], dst, s_recv.at[source]).start()

            @pl.when(h != m)
            def _():
                far.start()
        else:
            far.start()

    spot = spot_of(z, h)
    own_block = (spot * blocks + n - 1) // n
    busy = jnp.logical_and(own_block < blocks, (n * own_block) // blocks == spot)
    lane_acc[...] = jnp.zeros_like(lane_acc)

    def all_pieces(ref, sems):
        for jj in range(n // 2):
            for t in range(2):
                landed(
                    ref.at[pl.ds(t * half, half), pl.ds(jj * LANE, LANE)],
                    sems.at[(2 * jj + h) * 2 + t],
                )

    def place_of(block, quarter):
        high = BLK // QUARTERS
        return raws[quarter].at[
            pl.ds(pl.multiple_of((block // cols) * high, high), high),
            pl.ds(pl.multiple_of(lax.rem(block, cols) * BLK, BLK), BLK),
        ]

    def quarter_of(quarter):
        high = BLK // QUARTERS
        return upd.at[pl.ds(quarter * high, high)]

    def own_moves(quarter):
        block = jnp.minimum(own_block, blocks - 1)
        src, dst = quarter_of(quarter), place_of(block, quarter)
        return (
            remote(src, dst, gs_r.at[block, quarter], gr_r.at[block, quarter], dp=right),
            remote(src, dst, gs_l.at[block, quarter], gr_l.at[block, quarter], dp=left),
            pltpu.make_async_copy(src, dst, loc.at[2 + quarter]),
        )

    home_slot = packed[0, jnp.minimum(own_block, blocks - 1)] & SLOT_MASK

    for one in ring:
        one.wait_send()
    gt, m0 = a_all.at[pl.ds(0, BLK)], a_all.at[pl.ds(BLK, BLK)]

    @pl.when(busy)
    def _():
        all_pieces(home_g, h_recv)
        quartic, order_p, damping = picks_of(codes_at(home_slot))
        trace = trace_and_turn(home_g, gt, lane_acc)
        root_into(home_g, roots.at[0], order_p, quartic, damping, trace, None, m0, t0, q, r)
        root_into(home_g, roots.at[1], order_p, quartic, damping, trace, gt, m0, t0, q, r)

        def halve(at):
            span = pl.ds(at, STRIPE)
            q[span, :] = dot32(roots[0, span, :], home_g[...]).astype(jnp.bfloat16)

        over_stripes(BLK, halve)
        lane_acc[...] = jnp.zeros_like(lane_acc)

        def finish(at):
            span = pl.ds(at, STRIPE)
            block = dot32(q[span, :], roots[1]).astype(jnp.bfloat16)
            upd[span, :] = block
            wide = block.astype(jnp.float32)
            lane_acc[...] += jnp.sum((wide * wide).reshape(STRIPE // 8, 8, BLK), axis=0)

        over_stripes(BLK, finish)
        for quarter in range(QUARTERS):
            for one in own_moves(quarter):
                one.start()

    tile = lane_acc[:, :LANE]
    for part in range(1, BLK // LANE):
        tile = tile + lane_acc[:, part * LANE:(part + 1) * LANE]
    part_out[...] = tile
    parts[source] = tile

    def hops(side, quarter):
        return n // 2 if (quarter < QUARTERS // 2) == (side == 0) else n // 2 - 1

    def right_block(i):
        x = lax.rem(spot + n - 1, n)
        block = lax.rem(((x + 1) * blocks - 1) // n + blocks - i, blocks)
        return block, lax.rem(spot + n - (n * block) // blocks, n)

    def left_block(i):
        block = lax.rem(((spot + 1) * blocks - 1) // n + 1 + i, blocks)
        return block, lax.rem((n * block) // blocks + n - spot, n)

    def stream(i, quarter, side, phase):
        block, far = (right_block if side == 0 else left_block)(i)
        limit = hops(side, quarter)
        recv = (gr_r if side == 0 else gr_l).at[block, quarter]
        send = (gs_r if side == 0 else gs_l).at[block, quarter]
        ref = place_of(block, quarter)
        go = remote(ref, ref, send, recv, dp=right if side == 0 else left)
        if phase == 0:
            @pl.when(far < limit)
            def _():
                landed(ref, recv)
                go.start()
        elif phase == 1:
            @pl.when(far == limit)
            def _():
                landed(ref, recv)
        else:
            @pl.when(far < limit)
            def _():
                go.wait_send()

    slot_vals = {}

    def slot_first():
        all_pieces(slot_g, s_recv)
        slot_vals["picks"] = picks_of(codes_at(z))
        slot_vals["trace"] = trace_and_turn(slot_g, gt, lane_acc)

    def slot_unit(side, body):
        def run():
            quartic, order_p, damping = slot_vals["picks"]
            root_into(
                slot_g, roots.at[side], order_p, quartic, damping, slot_vals["trace"],
                None if side == 0 else gt, m0, t0, q, r, only=body,
            )
        return run

    units = [slot_first] + [slot_unit(side, body) for side in range(2) for body in range(5)]

    def part_move(o, t):
        return remote(
            part_out, parts.at[source], p_send.at[o, t], p_recv.at[source],
            dp=lax.rem(z + o, n), mp=t,
        )

    def part_each(act):
        remote_self = remote(
            part_out, parts.at[source], p_send.at[0, 0], p_recv.at[source], mp=1 - h
        )
        act(remote_self)
        for o in range(1, n):
            for t in range(2):
                act(part_move(o, t))

    most = (blocks + 1) // 2
    for i in range(most):
        for quarter in range(QUARTERS):
            stream(i, quarter, 0, 0)
            stream(i, quarter, 1, 0)
            if i == 0 and quarter == 0:
                part_each(lambda go: go.start())
            if i > 0 and units:
                units.pop(0)()
    for unit in units:
        unit()
    for i in range(most):
        for quarter in range(QUARTERS):
            stream(i, quarter, 0, 1)
            stream(i, quarter, 1, 1)

    for o in range(1, n):
        chip = lax.rem(z + o, n)
        for t in range(2):
            landed(parts.at[chip * 2 + t], p_recv.at[chip * 2 + t])
    landed(parts.at[z * 2 + 1 - h], p_recv.at[z * 2 + 1 - h])
    part_each(lambda go: go.wait_send())
    for o in range(n):
        piece_go(o, False)
        at = lax.rem(z + o, n)
        remote(b_all.at[at, h], b_all.at[at, h], f_send.at[at], f_recv.at[at], mp=1 - h).wait_send()
        home_go(o, False)
        chip, dst, far = slot_move(o)
        if o == 0:
            @pl.when(h != m)
            def _():
                far.wait_send()
        else:
            far.wait_send()

    @pl.when(busy)
    def _():
        for quarter in range(QUARTERS):
            one, two, local = own_moves(quarter)
            one.wait_send()
            two.wait_send()
            local.wait()

    for i in range(most):
        for quarter in range(QUARTERS):
            stream(i, quarter, 0, 2)
            stream(i, quarter, 1, 2)


def run_step(packed, activations, out_grads, n, rows, cols, devices):
    tok = activations.shape[0]
    dma = pltpu.SemaphoreType.DMA
    smem = pl.BlockSpec(memory_space=pltpu.SMEM)
    vmem = pl.BlockSpec(memory_space=pltpu.VMEM)
    hbm = pl.BlockSpec(memory_space=pltpu.HBM)
    blocks = rows * cols
    half = BLK // 2
    width = rows * half
    pieces = BLK // LANE
    bf = lambda *shape: pltpu.VMEM(shape, jnp.bfloat16)
    steps = n // 2
    return pl.pallas_call(
        functools.partial(step_kernel, n, rows, cols),
        out_shape=(
            *[jax.ShapeDtypeStruct((rows * BLK // QUARTERS, cols * BLK), jnp.bfloat16)] * QUARTERS,
            jax.ShapeDtypeStruct((2, BLK, BLK), jnp.bfloat16),
            jax.ShapeDtypeStruct((2 * n, 8, LANE), jnp.float32),
        ),
        in_specs=[smem, hbm, hbm],
        out_specs=(*[pl.BlockSpec(memory_space=pl.ANY)] * QUARTERS, vmem, vmem),
        scratch_shapes=[
            bf(n * tok, width), bf(pieces, tok, cols * LANE), bf(n, 2, tok // 2, cols * LANE),
            pltpu.VMEM((8, LANE), jnp.int32), pltpu.VMEM((8, LANE), jnp.int32), pltpu.SMEM((8, LANE), jnp.int32),
            pltpu.VMEM((width, cols * LANE), jnp.float32),
            bf(blocks, half, LANE), bf(n, half, LANE), bf(BLK, BLK), bf(BLK, BLK), bf(BLK, BLK),
            pltpu.VMEM((8, LANE), jnp.float32),
            bf(BLK, BLK), bf(BLK, BLK), bf(BLK, BLK),
            pltpu.VMEM((8, BLK), jnp.float32),
            dma((steps, rows)), dma((steps, rows)), dma((steps, rows)), dma((steps, rows)),
            dma((n, 2)), dma((n,)), dma((n,)), dma((n,)), dma(()), dma(()),
            dma((2 + QUARTERS,)),
            dma((n,)), dma((2 * n,)), dma((n,)), dma((2 * n,)), dma((n, 2)), dma((2 * n,)),
            dma((blocks, QUARTERS)), dma((blocks, QUARTERS)),
            dma((blocks, QUARTERS)), dma((blocks, QUARTERS)), dma((pieces, cols)),
            pltpu.SemaphoreType.REGULAR((steps,)), pltpu.SemaphoreType.REGULAR((steps,)),
        ],
        compiler_params=pltpu.CompilerParams(
            collective_id=1, has_side_effects=True, vmem_limit_bytes=VMEM_BASE + VMEM_PER_DEVICE * devices
        ),
        name="shampoo_step",
    )(packed, activations, out_grads)


def rescale_kernel(entries, high, parts, roots, *refs):
    raws, (out, roots_out, buffers, sems, root_sem) = refs[:QUARTERS], refs[QUARTERS:]
    root_copy = pltpu.make_async_copy(roots, roots_out, root_sem)
    root_copy.start()
    total_sq = jnp.sum(jnp.sum(parts[...], axis=0), keepdims=True)
    scale = lax.rsqrt(total_sq / entries + 1.0)
    groups = raws[0].shape[0] // high
    per_row = BLK // QUARTERS // high

    def out_copy(quarter, group):
        at = (group // per_row) * BLK + quarter * (BLK // QUARTERS) + lax.rem(group, per_row) * high
        return pltpu.make_async_copy(
            buffers.at[group], out.at[pl.ds(pl.multiple_of(at, high), high)], sems.at[group]
        )

    for quarter in range(QUARTERS):
        def step(group, carry, quarter=quarter):
            if quarter > 0:
                out_copy(quarter - 1, group).wait()
            span = pl.ds(pl.multiple_of(group * high, high), high)
            wide = raws[quarter][span, :].astype(jnp.float32)
            buffers[group] = (wide * scale).astype(jnp.bfloat16)
            out_copy(quarter, group).start()
            return carry

        lax.fori_loop(0, groups, step, 0)
    for group in range(groups):
        out_copy(QUARTERS - 1, group).wait()
    root_copy.wait()


def rescaled(raws, parts, roots, entries, devices):
    height, width = raws[0].shape
    high = BLK // QUARTERS // 2
    vmem = pl.BlockSpec(memory_space=pltpu.VMEM)
    return pl.pallas_call(
        functools.partial(rescale_kernel, entries, high),
        out_shape=(
            jax.ShapeDtypeStruct((height * QUARTERS, width), jnp.bfloat16),
            jax.ShapeDtypeStruct(roots.shape, jnp.bfloat16),
        ),
        in_specs=[vmem] * (2 + QUARTERS),
        out_specs=(pl.BlockSpec(memory_space=pltpu.HBM), pl.BlockSpec(memory_space=pltpu.HBM)),
        scratch_shapes=[
            pltpu.VMEM((height // high, high, width), jnp.bfloat16),
            pltpu.SemaphoreType.DMA((height // high,)),
            pltpu.SemaphoreType.DMA(()),
        ],
        compiler_params=pltpu.CompilerParams(vmem_limit_bytes=RESCALE_BASE + VMEM_PER_DEVICE * devices),
        cost_estimate=pl.CostEstimate(
            flops=8 * height * width, bytes_accessed=16 * height * width, transcendentals=0
        ),
        name="rescaled",
    )(parts, roots, *raws)


def on_device(devices, activations, out_grads, slot_table, exponent_index, damping_index):
    n = lax.axis_size("dp")
    rows = activations.shape[1] // BLK
    cols = out_grads.shape[1] // BLK
    *raws, roots, parts = run_step(
        slot_table + exponent_index * 256 + damping_index * 4096, activations, out_grads, n, rows, cols, devices
    )
    entries = rows * BLK * cols * BLK * lax.axis_size("mp")
    update, roots = rescaled(raws, parts, roots, float(entries), devices)
    return (update, roots[None, None])


def solution(mesh):
    placed = (
        P(("member", "dp"), None),
        P(("member", "dp"), "mp"),
        P(("member", "mp"), None),
        P(("member", "mp"), None),
        P(("member", "mp"), None),
    )
    return jax.shard_map(
        functools.partial(on_device, mesh.size),
        mesh=mesh,
        in_specs=placed,
        out_specs=(P("member", "mp"), P(("member", "mp"), "dp", None, None, None)),
        check_vma=False,
    )
```

```python
import functools

import jax
import jax.numpy as jnp
import numpy as np
from jax import lax
from jax.experimental import pallas as pl
from jax.experimental.pallas import tpu as pltpu
from jax.sharding import PartitionSpec as P

BLK = 1024
LANE = 128
ROOT_ORDERS = (2.0, 4.0)
DAMPINGS = (0.03, 0.1, 0.3, 1.0)
SHIFT = 4
MESH = pl.DeviceIdType.MESH


STRIPE = 256


def eye_stripe(at, size):
    row = lax.broadcasted_iota(jnp.int32, (STRIPE, size), 0) + at
    col = lax.broadcasted_iota(jnp.int32, (STRIPE, size), 1)
    return row == col


def dot32(first, second, dims=((1,), (0,))):
    return lax.dot_general(first, second, (dims, ((), ())), preferred_element_type=jnp.float32)


def over_stripes(size, body):
    def step(index, carry):
        body(pl.multiple_of(index * STRIPE, STRIPE))
        return carry

    lax.fori_loop(0, size // STRIPE, step, 0)


def root_into(g, root, order, quartic, damping, trace, gt, m0, t0, q, r, only=None):
    size = g.shape[0]
    shift = damping * (trace / size + 1.0)
    ratio = size / (2.0 * (trace + shift * size))
    base = g if gt is None else gt

    def stat(at):
        rows = pl.ds(at, STRIPE)
        s = dot32(base[rows, :], base[...], ((1,), (1,)))
        on = eye_stripe(at, size)
        scaled = jnp.where(on, s + shift, s) * ratio
        m0[rows, :] = scaled.astype(jnp.bfloat16)
        t0[rows, :] = (jnp.where(on, (order + 1.0) - scaled, -scaled) / order).astype(jnp.bfloat16)

    def square(at):
        rows = pl.ds(at, STRIPE)
        q[rows, :] = dot32(t0[rows, :], t0[...]).astype(jnp.bfloat16)

    def fourth(at):
        rows = pl.ds(at, STRIPE)
        f = dot32(q[rows, :], q[...])
        r[rows, :] = jnp.where(quartic, f, q[rows, :].astype(jnp.float32)).astype(jnp.bfloat16)

    def factor(at):
        rows = pl.ds(at, STRIPE)
        m = dot32(r[rows, :], m0[...])
        on = eye_stripe(at, size)
        q[rows, :] = (jnp.where(on, (order + 1.0) - m, -m) / order).astype(jnp.bfloat16)

    def last(at):
        rows = pl.ds(at, STRIPE)
        root[rows, :] = dot32(t0[rows, :], q[...]).astype(jnp.bfloat16)

    for index, body in enumerate((stat, square, fourth, factor, last)):
        if only is None or only == index:
            over_stripes(size, body)


def trace_and_turn(g, gt, acc):
    size = g.shape[0]
    acc[...] = jnp.zeros_like(acc)

    def body(at):
        rows = pl.ds(at, STRIPE)
        part = g[rows, :]
        wide = part.astype(jnp.float32)
        acc[...] += jnp.sum((wide * wide).reshape(STRIPE // 8, 8, size), axis=0)
        gt[:, rows] = part.T

    over_stripes(size, body)
    return jnp.sum(acc[...])


def picks_of(codes):
    quartic = codes[0] == 1
    order = jnp.where(quartic, ROOT_ORDERS[1], ROOT_ORDERS[0])
    damping = jnp.float32(DAMPINGS[0])
    for index in range(1, len(DAMPINGS)):
        damping = jnp.where(codes[1] == index, jnp.float32(DAMPINGS[index]), damping)
    return quartic, order, damping


def greet_neighbours(n, z, h):
    barrier = pltpu.get_barrier_semaphore()
    pl.semaphore_signal(barrier, inc=1, device_id={"mp": 1 - h}, device_id_type=MESH)
    for o in (1, n - 1):
        pl.semaphore_signal(
            barrier, inc=1, device_id={"dp": lax.rem(z + o, n)}, device_id_type=MESH
        )
    pl.semaphore_wait(barrier, 3)


def remote(src, dst, send, recv, **to):
    return pltpu.make_async_remote_copy(
        src_ref=src, dst_ref=dst, send_sem=send, recv_sem=recv, device_id=to, device_id_type=MESH
    )


def landed(ref, sem):
    pltpu.make_async_copy(ref, ref, sem).wait()


def both_ways(n):
    order = [n // 2]
    for o in range(n // 2 - 1, 0, -1):
        order.extend([o, n - o])
    return order + [0]


QUARTERS = 8
SLOT_MASK = 255
VMEM_BASE = 27 << 20
VMEM_PER_DEVICE = 7 << 10
RESCALE_BASE = 22 << 20


def step_kernel(
    n, rows, cols,
    packed, act, grads,
    *refs,
):
    raws = refs[:QUARTERS]
    (
        roots, parts, a_all, b_in, b_all, table_in, table_far, table_smem, acc, shard,
        payload, home_g, slot_g, upd, part_out, t0, q, r, lane_acc, as_r, ar_r,
        as_l, ar_l, b_send, b_recv, f_send, f_recv, t_send, t_recv, loc, h_send, h_recv,
        s_send, s_recv, p_send, p_recv, gs_r, gr_r, gs_l, gr_l, b_load, tok_r, tok_l,
    ) = refs[QUARTERS:]
    z = lax.axis_index("dp")
    h = lax.axis_index("mp")
    blocks = rows * cols
    tok = act.shape[0]
    half_tok = tok // 2
    half = BLK // 2
    pieces = BLK // LANE
    loads = []

    def chunk(at):
        return a_all.at[pl.ds(pl.multiple_of(at * tok, tok), tok)]

    for row in range(rows):
        span = pl.ds(pl.multiple_of(row * BLK + h * half, half), half)
        loads.append(pltpu.make_async_copy(
            act.at[:, span], chunk(z).at[:, pl.ds(row * half, half)], loc.at[row]
        ))
    for col in range(cols):
        for jj in range(pieces):
            loads.append(pltpu.make_async_copy(
                grads.at[:, pl.ds(col * BLK + jj * LANE, LANE)],
                b_in.at[jj, :, pl.ds(col * LANE, LANE)],
                b_load.at[jj, col],
            ))
    for one in loads:
        one.start()
    def codes_at(slot):
        word = packed[0, slot]
        return (word >> 8) & 15, (word >> 12) & 15

    lane = lax.broadcasted_iota(jnp.int32, (8, LANE), 1)
    line = jnp.zeros((8, LANE), jnp.int32)
    for block in range(blocks):
        line = jnp.where(lane == block, packed[0, block] & SLOT_MASK, line)
    table_in[...] = line
    right, left = lax.rem(z + 1, n), lax.rem(z + n - 1, n)
    steps = n // 2
    greet_neighbours(n, z, h)

    def tell(t):
        pl.semaphore_signal(tok_r.at[t], inc=1, device_id={"dp": right}, device_id_type=MESH)
        if t < steps - 1:
            pl.semaphore_signal(tok_l.at[t], inc=1, device_id={"dp": left}, device_id_type=MESH)

    def hear(t):
        pl.semaphore_wait(tok_r.at[t], 1)
        if t < steps - 1:
            pl.semaphore_wait(tok_l.at[t], 1)

    tell(0)

    ring = []
    for one in loads:
        one.wait()

    def ring_part(at, row):
        return chunk(at).at[:, pl.ds(row * half, half)]

    def ring_rows(step, side):
        return (side,) if step == steps - 1 else tuple(range(rows))

    def ring_send(step, side, row):
        at = lax.rem(z + n - step, n) if side == 0 else lax.rem(z + step, n)
        ref = ring_part(at, row)
        send, recv, to = (as_r, ar_r, right) if side == 0 else (as_l, ar_l, left)
        one = remote(ref, ref, send.at[step, row], recv.at[step, row], dp=to)
        one.start()
        ring.append(one)

    def ring_recv(step, side, row):
        at = lax.rem(z + n - step - 1, n) if side == 0 else lax.rem(z + step + 1, n)
        landed(ring_part(at, row), (ar_r if side == 0 else ar_l).at[step, row])

    table = remote(table_in, table_far, t_send, t_recv, mp=1 - h)
    table.start()
    for row in range(rows):
        for side in range(2):
            ring_send(0, side, row)
    parity = lax.rem(z + h, 2)
    h_rows = pl.ds(pl.multiple_of(h * half_tok, half_tok), half_tok)
    o_rows = pl.ds(pl.multiple_of((1 - h) * half_tok, half_tok), half_tok)

    def piece(o):
        chip = lax.rem(z + o, n)
        block = b_in.at[chip // 2]
        same = remote(block.at[h_rows], b_all.at[z, h], b_send.at[o, 0], b_recv.at[z], dp=chip, mp=h)
        other = remote(
            block.at[o_rows], b_all.at[z, 1 - h], b_send.at[o, 1], b_recv.at[z], dp=chip, mp=1 - h
        )
        return same, other

    def piece_go(o, start):
        @pl.when(parity == o % 2)
        def _():
            same, other = piece(o)
            if o == 0:
                if start:
                    pltpu.make_async_copy(
                        b_in.at[z // 2].at[h_rows], b_all.at[z, h], b_recv.at[z]
                    ).start()
            elif start:
                same.start()
            else:
                same.wait_send()
            if start:
                other.start()
            else:
                other.wait_send()

    piece_go(0, True)
    for t in range(steps):
        hear(t)
        if t < steps - 1:
            tell(t + 1)
            piece_go(t + 1, True)
            piece_go(n - t - 1, True)
        else:
            piece_go(steps, True)

    def forward(at):
        landed(b_all.at[at, h], b_recv.at[at])
        remote(b_all.at[at, h], b_all.at[at, h], f_send.at[at], f_recv.at[at], mp=1 - h).start()

    def add_source(at, fresh=False):
        landed(b_all.at[at, 1 - h], f_recv.at[at])

        right_side = b_all[at].reshape(tok, cols * LANE)
        for row in range(rows):
            got = dot32(
                chunk(at)[:, row * half:(row + 1) * half], right_side, ((0,), (0,))
            )
            span = pl.ds(row * half, half)
            if fresh:
                acc[span, :] = got
            else:
                acc[span, :] += got

    forward(z)
    for step in range(steps):
        if step == steps - 1:
            add_source(lax.rem(z + step, n))
            add_source(lax.rem(z + n - step, n))
        for row in range(rows):
            for side in range(2):
                if row in ring_rows(step, side):
                    ring_recv(step, side, row)
                if step < steps - 1 and row in ring_rows(step + 1, side):
                    ring_send(step + 1, side, row)
        if step == steps - 1:
            forward(lax.rem(z + steps, n))
        else:
            forward(lax.rem(z + step + 1, n))
            forward(lax.rem(z + n - step - 1, n))
        if step == 0:
            add_source(z, True)
        elif step < steps - 1:
            add_source(lax.rem(z + step, n))
            add_source(lax.rem(z + n - step, n))
    add_source(lax.rem(z + steps, n))
    for row in range(rows):
        for col in range(cols):
            shard[row * cols + col] = acc[
                row * half:(row + 1) * half, col * LANE:(col + 1) * LANE
            ].astype(jnp.bfloat16)

    m = lax.rem(z, 2)
    j = z // 2
    source = z * 2 + h
    spot_of = lambda chip, side: lax.rem(chip + n - SHIFT * side, n)
    my_rows = pl.ds(pl.multiple_of(h * half, half), half)
    my_cols = pl.ds(pl.multiple_of(j * LANE, LANE), LANE)

    def home_move(o):
        chip = lax.rem(z + o, n)
        at = spot_of(chip, m)
        block = (at * blocks + n - 1) // n
        used = jnp.logical_and(block < blocks, (n * block) // blocks == at)
        block = jnp.minimum(block, blocks - 1)
        dst = home_g.at[my_rows, my_cols]
        far = remote(shard.at[block], dst, h_send.at[o], h_recv.at[source], dp=chip, mp=m)
        return used, block, dst, far

    def home_go(o, start):
        used, block, dst, far = home_move(o)
        if o == 0:
            if start:
                @pl.when(jnp.logical_and(used, h == m))
                def _():
                    pltpu.make_async_copy(shard.at[block], dst, h_recv.at[source]).start()

            used = jnp.logical_and(used, h != m)

        @pl.when(used)
        def _():
            if start:
                far.start()
            else:
                far.wait_send()

    for o in both_ways(n):
        home_go(o, True)

    table.wait()
    to_smem = pltpu.make_async_copy(table_far, table_smem, loc.at[1])
    to_smem.start()
    to_smem.wait()

    def slot_move(o):
        chip = lax.rem(z + o, n)
        dst = slot_g.at[my_rows, my_cols]
        return chip, dst, remote(payload.at[chip], dst, s_send.at[o], s_recv.at[source], dp=chip, mp=m)

    for slot in range(n):
        pick = jnp.int32(0)
        filled = jnp.int32(0)
        for block in range(blocks):
            served = jnp.where(m == h, packed[0, block] & SLOT_MASK, table_smem[0, block])
            pick = jnp.where(served == slot, block, pick)
            filled = jnp.where(served == slot, 1, filled)
        part = shard[pick]
        payload[slot] = jnp.where(filled == 1, part, jnp.zeros_like(part))
    for o in both_ways(n):
        chip, dst, far = slot_move(o)
        if o == 0:
            @pl.when(h == m)
            def _():
                pltpu.make_async_copy(payload.at[chip], dst, s_recv.at[source]).start()

            @pl.when(h != m)
            def _():
                far.start()
        else:
            far.start()

    spot = spot_of(z, h)
    own_block = (spot * blocks + n - 1) // n
    busy = jnp.logical_and(own_block < blocks, (n * own_block) // blocks == spot)
    lane_acc[...] = jnp.zeros_like(lane_acc)

    def all_pieces(ref, sems):
        for jj in range(n // 2):
            for t in range(2):
                landed(
                    ref.at[pl.ds(t * half, half), pl.ds(jj * LANE, LANE)],
                    sems.at[(2 * jj + h) * 2 + t],
                )

    def place_of(block, quarter):
        high = BLK // QUARTERS
        return raws[quarter].at[
            pl.ds(pl.multiple_of((block // cols) * high, high), high),
            pl.ds(pl.multiple_of(lax.rem(block, cols) * BLK, BLK), BLK),
        ]

    def quarter_of(quarter):
        high = BLK // QUARTERS
        return upd.at[pl.ds(quarter * high, high)]

    def own_moves(quarter):
        block = jnp.minimum(own_block, blocks - 1)
        src, dst = quarter_of(quarter), place_of(block, quarter)
        return (
            remote(src, dst, gs_r.at[block, quarter], gr_r.at[block, quarter], dp=right),
            remote(src, dst, gs_l.at[block, quarter], gr_l.at[block, quarter], dp=left),
            pltpu.make_async_copy(src, dst, loc.at[2 + quarter]),
        )

    home_slot = packed[0, jnp.minimum(own_block, blocks - 1)] & SLOT_MASK

    for one in ring:
        one.wait_send()
    gt, m0 = a_all.at[pl.ds(0, BLK)], a_all.at[pl.ds(BLK, BLK)]

    @pl.when(busy)
    def _():
        all_pieces(home_g, h_recv)
        quartic, order_p, damping = picks_of(codes_at(home_slot))
        trace = trace_and_turn(home_g, gt, lane_acc)
        root_into(home_g, roots.at[0], order_p, quartic, damping, trace, None, m0, t0, q, r)
        root_into(home_g, roots.at[1], order_p, quartic, damping, trace, gt, m0, t0, q, r)

        def halve(at):
            span = pl.ds(at, STRIPE)
            q[span, :] = dot32(roots[0, span, :], home_g[...]).astype(jnp.bfloat16)

        over_stripes(BLK, halve)
        lane_acc[...] = jnp.zeros_like(lane_acc)

        def finish(at):
            span = pl.ds(at, STRIPE)
            block = dot32(q[span, :], roots[1]).astype(jnp.bfloat16)
            upd[span, :] = block
            wide = block.astype(jnp.float32)
            lane_acc[...] += jnp.sum((wide * wide).reshape(STRIPE // 8, 8, BLK), axis=0)

        over_stripes(BLK, finish)
        for quarter in range(QUARTERS):
            for one in own_moves(quarter):
                one.start()

    tile = lane_acc[:, :LANE]
    for part in range(1, BLK // LANE):
        tile = tile + lane_acc[:, part * LANE:(part + 1) * LANE]
    part_out[...] = tile
    parts[source] = tile

    def hops(side, quarter):
        return n // 2 if (quarter < QUARTERS // 2) == (side == 0) else n // 2 - 1

    def right_block(i):
        x = lax.rem(spot + n - 1, n)
        block = lax.rem(((x + 1) * blocks - 1) // n + blocks - i, blocks)
        return block, lax.rem(spot + n - (n * block) // blocks, n)

    def left_block(i):
        block = lax.rem(((spot + 1) * blocks - 1) // n + 1 + i, blocks)
        return block, lax.rem((n * block) // blocks + n - spot, n)

    def stream(i, quarter, side, phase):
        block, far = (right_block if side == 0 else left_block)(i)
        limit = hops(side, quarter)
        recv = (gr_r if side == 0 else gr_l).at[block, quarter]
        send = (gs_r if side == 0 else gs_l).at[block, quarter]
        ref = place_of(block, quarter)
        go = remote(ref, ref, send, recv, dp=right if side == 0 else left)
        if phase == 0:
            @pl.when(far < limit)
            def _():
                landed(ref, recv)
                go.start()
        elif phase == 1:
            @pl.when(far == limit)
            def _():
                landed(ref, recv)
        else:
            @pl.when(far < limit)
            def _():
                go.wait_send()

    slot_vals = {}

    def slot_first():
        all_pieces(slot_g, s_recv)
        slot_vals["picks"] = picks_of(codes_at(z))
        slot_vals["trace"] = trace_and_turn(slot_g, gt, lane_acc)

    def slot_unit(side, body):
        def run():
            quartic, order_p, damping = slot_vals["picks"]
            root_into(
                slot_g, roots.at[side], order_p, quartic, damping, slot_vals["trace"],
                None if side == 0 else gt, m0, t0, q, r, only=body,
            )
        return run

    units = [slot_first] + [slot_unit(side, body) for side in range(2) for body in range(5)]

    def part_move(o, t):
        return remote(
            part_out, parts.at[source], p_send.at[o, t], p_recv.at[source],
            dp=lax.rem(z + o, n), mp=t,
        )

    def part_each(act):
        remote_self = remote(
            part_out, parts.at[source], p_send.at[0, 0], p_recv.at[source], mp=1 - h
        )
        act(remote_self)
        for o in range(1, n):
            for t in range(2):
                act(part_move(o, t))

    most = (blocks + 1) // 2
    for i in range(most):
        for quarter in range(QUARTERS):
            stream(i, quarter, 0, 0)
            stream(i, quarter, 1, 0)
            if i == 0 and quarter == 0:
                part_each(lambda go: go.start())
            if i > 0 and units:
                units.pop(0)()
    for unit in units:
        unit()
    for i in range(most):
        for quarter in range(QUARTERS):
            stream(i, quarter, 0, 1)
            stream(i, quarter, 1, 1)

    for o in range(1, n):
        chip = lax.rem(z + o, n)
        for t in range(2):
            landed(parts.at[chip * 2 + t], p_recv.at[chip * 2 + t])
    landed(parts.at[z * 2 + 1 - h], p_recv.at[z * 2 + 1 - h])
    part_each(lambda go: go.wait_send())
    for o in range(n):
        piece_go(o, False)
        at = lax.rem(z + o, n)
        remote(b_all.at[at, h], b_all.at[at, h], f_send.at[at], f_recv.at[at], mp=1 - h).wait_send()
        home_go(o, False)
        chip, dst, far = slot_move(o)
        if o == 0:
            @pl.when(h != m)
            def _():
                far.wait_send()
        else:
            far.wait_send()

    @pl.when(busy)
    def _():
        for quarter in range(QUARTERS):
            one, two, local = own_moves(quarter)
            one.wait_send()
            two.wait_send()
            local.wait()

    for i in range(most):
        for quarter in range(QUARTERS):
            stream(i, quarter, 0, 2)
            stream(i, quarter, 1, 2)


def run_step(packed, activations, out_grads, n, rows, cols, devices):
    tok = activations.shape[0]
    dma = pltpu.SemaphoreType.DMA
    smem = pl.BlockSpec(memory_space=pltpu.SMEM)
    vmem = pl.BlockSpec(memory_space=pltpu.VMEM)
    hbm = pl.BlockSpec(memory_space=pltpu.HBM)
    blocks = rows * cols
    half = BLK // 2
    width = rows * half
    pieces = BLK // LANE
    bf = lambda *shape: pltpu.VMEM(shape, jnp.bfloat16)
    steps = n // 2
    return pl.pallas_call(
        functools.partial(step_kernel, n, rows, cols),
        out_shape=(
            *[jax.ShapeDtypeStruct((rows * BLK // QUARTERS, cols * BLK), jnp.bfloat16)] * QUARTERS,
            jax.ShapeDtypeStruct((2, BLK, BLK), jnp.bfloat16),
            jax.ShapeDtypeStruct((2 * n, 8, LANE), jnp.float32),
        ),
        in_specs=[smem, hbm, hbm],
        out_specs=(*[pl.BlockSpec(memory_space=pl.ANY)] * QUARTERS, vmem, vmem),
        scratch_shapes=[
            bf(n * tok, width), bf(pieces, tok, cols * LANE), bf(n, 2, tok // 2, cols * LANE),
            pltpu.VMEM((8, LANE), jnp.int32), pltpu.VMEM((8, LANE), jnp.int32), pltpu.SMEM((8, LANE), jnp.int32),
            pltpu.VMEM((width, cols * LANE), jnp.float32),
            bf(blocks, half, LANE), bf(n, half, LANE), bf(BLK, BLK), bf(BLK, BLK), bf(BLK, BLK),
            pltpu.VMEM((8, LANE), jnp.float32),
            bf(BLK, BLK), bf(BLK, BLK), bf(BLK, BLK),
            pltpu.VMEM((8, BLK), jnp.float32),
            dma((steps, rows)), dma((steps, rows)), dma((steps, rows)), dma((steps, rows)),
            dma((n, 2)), dma((n,)), dma((n,)), dma((n,)), dma(()), dma(()),
            dma((2 + QUARTERS,)),
            dma((n,)), dma((2 * n,)), dma((n,)), dma((2 * n,)), dma((n, 2)), dma((2 * n,)),
            dma((blocks, QUARTERS)), dma((blocks, QUARTERS)),
            dma((blocks, QUARTERS)), dma((blocks, QUARTERS)), dma((pieces, cols)),
            pltpu.SemaphoreType.REGULAR((steps,)), pltpu.SemaphoreType.REGULAR((steps,)),
        ],
        compiler_params=pltpu.CompilerParams(
            collective_id=1, has_side_effects=True, vmem_limit_bytes=VMEM_BASE + VMEM_PER_DEVICE * devices
        ),
        name="shampoo_step",
    )(packed, activations, out_grads)


def rescale_kernel(entries, high, parts, roots, *refs):
    raws, (out, roots_out, buffers, sems, root_sem) = refs[:QUARTERS], refs[QUARTERS:]
    root_copy = pltpu.make_async_copy(roots, roots_out, root_sem)
    root_copy.start()
    total_sq = jnp.sum(jnp.sum(parts[...], axis=0), keepdims=True)
    scale = lax.rsqrt(total_sq / entries + 1.0)
    groups = raws[0].shape[0] // high
    per_row = BLK // QUARTERS // high

    def out_copy(quarter, group):
        at = (group // per_row) * BLK + quarter * (BLK // QUARTERS) + lax.rem(group, per_row) * high
        return pltpu.make_async_copy(
            buffers.at[group], out.at[pl.ds(pl.multiple_of(at, high), high)], sems.at[group]
        )

    for quarter in range(QUARTERS):
        def step(group, carry, quarter=quarter):
            if quarter > 0:
                out_copy(quarter - 1, group).wait()
            span = pl.ds(pl.multiple_of(group * high, high), high)
            wide = raws[quarter][span, :].astype(jnp.float32)
            buffers[group] = (wide * scale).astype(jnp.bfloat16)
            out_copy(quarter, group).start()
            return carry

        lax.fori_loop(0, groups, step, 0)
    for group in range(groups):
        out_copy(QUARTERS - 1, group).wait()
    root_copy.wait()


def rescaled(raws, parts, roots, entries, devices):
    height, width = raws[0].shape
    high = BLK // QUARTERS // 2
    vmem = pl.BlockSpec(memory_space=pltpu.VMEM)
    return pl.pallas_call(
        functools.partial(rescale_kernel, entries, high),
        out_shape=(
            jax.ShapeDtypeStruct((height * QUARTERS, width), jnp.bfloat16),
            jax.ShapeDtypeStruct(roots.shape, jnp.bfloat16),
        ),
        in_specs=[vmem] * (2 + QUARTERS),
        out_specs=(pl.BlockSpec(memory_space=pltpu.HBM), pl.BlockSpec(memory_space=pltpu.HBM)),
        scratch_shapes=[
            pltpu.VMEM((height // high, high, width), jnp.bfloat16),
            pltpu.SemaphoreType.DMA((height // high,)),
            pltpu.SemaphoreType.DMA(()),
        ],
        compiler_params=pltpu.CompilerParams(vmem_limit_bytes=RESCALE_BASE + VMEM_PER_DEVICE * devices),
        cost_estimate=pl.CostEstimate(
            flops=8 * height * width, bytes_accessed=16 * height * width, transcendentals=0
        ),
        name="rescaled",
    )(parts, roots, *raws)


def on_device(devices, activations, out_grads, slot_table, exponent_index, damping_index):
    n = lax.axis_size("dp")
    rows = activations.shape[1] // BLK
    cols = out_grads.shape[1] // BLK
    *raws, roots, parts = run_step(
        slot_table + exponent_index * 256 + damping_index * 4096, activations, out_grads, n, rows, cols, devices
    )
    entries = rows * BLK * cols * BLK * lax.axis_size("mp")
    update, roots = rescaled(raws, parts, roots, float(entries), devices)
    return (update, roots[None, None])


def solution(mesh):
    placed = (
        P(("member", "dp"), None),
        P(("member", "dp"), "mp"),
        P(("member", "mp"), None),
        P(("member", "mp"), None),
        P(("member", "mp"), None),
    )
    return jax.shard_map(
        functools.partial(on_device, mesh.size),
        mesh=mesh,
        in_specs=placed,
        out_specs=(P("member", "mp"), P(("member", "mp"), "dp", None, None, None)),
        check_vma=False,
    )
```
